32 devices in a mesh: dp: 8 (over y, x, core), tensor: 4 (over z).
Axes of the slice: x: 2, y: 2, z: 4, core: 2. Of those that a mesh axis runs over, the one named last changes fastest.
Arguments:
- hidden_in: bfloat16 [8192, 2048], P(('dp', 'tensor')), may hold values from -6 to 6
- ln_gain: bfloat16 [2048], P('dp'), may hold values from 0.25 to 1.75
- ln_bias: bfloat16 [2048], P('dp'), may hold values from -4 to 4
- qkv_weight: bfloat16 [2048, 3, 2048], P('dp', None, 'tensor'), may hold values from -0.125 to 0.125
- qkv_bias: bfloat16 [3, 32, 64], P(None, 'tensor', 'dp'), may hold values from -4 to 4
- dense_weight: bfloat16 [2048, 2048], P('tensor', 'dp'), may hold values from -0.5 to 0.5
- dense_bias: bfloat16 [2048], P('dp'), may hold values from -6 to 6
- fc1_weight: bfloat16 [2048, 8192], P('dp', 'tensor'), may hold values from -0.125 to 0.125
- fc1_bias: bfloat16 [128, 64], P('tensor', 'dp'), may hold values from -6 to 6
- fc2_weight: bfloat16 [8192, 2048], P('tensor', 'dp'), may hold values from -0.09375 to 0.09375
- fc2_bias: bfloat16 [2048], P('dp'), may hold values from -6 to 6
- cotangent: bfloat16 [8192, 2048], P(('dp', 'tensor')), may hold values from -6 to 6
Outputs:
- hidden_out: bfloat16 [8192, 2048], P(('dp', 'tensor'))
- input_grad: float32 [8192, 2048], P(('dp', 'tensor'))
- qkv_weight_grad: float32 [2048, 3, 2048], P('dp', None, 'tensor')
- qkv_bias_grad: float32 [3, 32, 64], P(None, 'tensor', 'dp')
- dense_weight_grad: float32 [2048, 2048], P('tensor', 'dp')
- dense_bias_grad: float32 [2048], P(('dp', 'tensor'))
- fc1_weight_grad: float32 [2048, 8192], P('dp', 'tensor')
- fc1_bias_grad: float32 [128, 64], P('tensor', 'dp')
- fc2_weight_grad: float32 [8192, 2048], P('tensor', 'dp')
- fc2_bias_grad: float32 [2048], P(('dp', 'tensor'))
- ln_gain_grad: float32 [2048], P(('dp', 'tensor'))
- ln_bias_grad: float32 [2048], P(('dp', 'tensor'))
The draws below stay inside these ranges and needn't reach their ends.
All inputs are finite; a program needn't handle non-finite values.
Results may differ from the reference program's by a relative error of at most 0.013.
Values may be sent and summed in bfloat16 or wider, within the bound.
A program may use at most 256 MiB of HBM per device.

```python
import math
import jax
import jax.numpy as jnp
from jax import lax

D = 2048
H = 32
HD = 64
ROT = 32
FF = 8192
LEN = 512
TOKENS = 8192


def spiked(entries, key, source, target, blocks, factor):
    def block_of(axis_at):
        return (jnp.arange(entries.shape[axis_at]) // (entries.shape[axis_at] // blocks)).reshape((-1,) + (1,) * (entries.ndim - 1 - axis_at))

    first = jax.random.permutation(key, blocks)[block_of(target)]
    other_side = (block_of(target) + blocks // 2) % blocks
    return jnp.where((block_of(source) == first) | (block_of(source) == other_side), factor * entries, entries)


def level_of(own_key, extent, split, smallest, largest):
    loudness, own = 1.0, jax.random.fold_in(own_key, 6)
    for axis_at, parts in split:
        draws = jnp.exp(jax.random.uniform(jax.random.fold_in(own, axis_at), (parts,), jnp.float32, smallest / len(split), largest / len(split)))
        loudness = loudness * jnp.repeat(draws, extent[axis_at] // parts).reshape([-1 if axis == axis_at else 1 for axis in range(len(extent))])
    return loudness


def normal_values(own_key, shape, deviation, reach, shards=(), dtype=jnp.bfloat16):
    loudness = level_of(own_key, shape, shards, -0.22, 0.18) if shards else 1.0
    result = jax.random.normal(own_key, shape, jnp.float32) * deviation * loudness
    return jnp.minimum(jnp.maximum(result, -reach), reach).astype(dtype)


def bell_draw_with(own_key, shape, spread, reach, shards, heavy, dtype=jnp.bfloat16):
    drawn = spread * jax.random.normal(own_key, shape, jnp.float32)
    if shards:
        drawn = drawn * level_of(own_key, shape, shards, -0.22, 0.18)
    return jnp.clip(spiked(drawn, jax.random.fold_in(own_key, 3), *heavy), -reach, reach).astype(dtype)


def setup_inputs(seed: int = 0) -> dict:
    seeds = jax.random.split(jax.random.key(seed), 13)
    return {
        "hidden_in": bell_draw_with(seeds[0], (TOKENS, D), 1.0, 6.0, ((0, 32),), (0, 1, 32, 2.75)),
        "ln_gain": jnp.clip(1.0 + 0.15 * jax.random.normal(seeds[1], (D,), jnp.float32), 0.25, 1.75).astype(jnp.bfloat16),
        "ln_bias": normal_values(seeds[2], (D,), 0.3, 4.0, ((0, 8),)),
        "qkv_weight": normal_values(seeds[3], (D, 3, D), D ** -0.5, 0.125, ((0, 8), (2, 4))),
        "qkv_bias": normal_values(seeds[4], (3, H, HD), 0.3, 4.0, ((1, 4), (2, 8))),
        "dense_weight": normal_values(seeds[5], (D, D), (D // 16) ** -0.5, 0.5, ((0, 4), (1, 8))),
        "dense_bias": normal_values(seeds[6], (D,), 0.5, 6.0, ((0, 8),)),
        "fc1_weight": normal_values(seeds[7], (D, FF), D ** -0.5, 0.125, ((0, 8), (1, 4))),
        "fc1_bias": normal_values(seeds[8], (FF // HD, HD), 0.5, 6.0, ((0, 4), (1, 8))),
        "fc2_weight": normal_values(seeds[9], (FF, D), (FF // 2) ** -0.5, 0.09375, ((0, 4), (1, 8))),
        "fc2_bias": normal_values(seeds[10], (D,), 0.5, 6.0, ((0, 8),)),
        "cotangent": bell_draw_with(seeds[11], (TOKENS, D), 1.0, 6.0, ((0, 32),), (0, 1, 32, 2.75)),
    }


EPSILON = 1e-05
GELU_C = math.sqrt(2.0 / math.pi)

def gelu_pair(hidden_pre):
    tanh_arg = GELU_C * (hidden_pre + 0.044715 * hidden_pre * hidden_pre * hidden_pre)
    tangent = jnp.tanh(tanh_arg)
    gelu_value = 0.5 * hidden_pre * (1.0 + tangent)
    gelu_slope = 0.5 * (1.0 + tangent) + 0.5 * hidden_pre * (1.0 - tangent * tangent) * GELU_C * (1.0 + 3.0 * 0.044715 * hidden_pre * hidden_pre)
    return (gelu_value, gelu_slope)

def rotary_tables(row_count):
    position = (jnp.arange(row_count) % LEN).astype(jnp.float32)
    frequency = 10000.0 ** (-jnp.arange(0, ROT, 2).astype(jnp.float32) / ROT)
    angles = position[:, None] * frequency[None, :]
    return (jnp.cos(angles)[:, None, :], jnp.sin(angles)[:, None, :])

def rotate(field_in, cosine, sine_table, sign_flip):
    half_rot = ROT // 2
    lower_half = field_in[..., :half_rot]
    upper_half = field_in[..., half_rot:ROT]
    return jnp.concatenate([lower_half * cosine - sign_flip * upper_half * sine_table, upper_half * cosine + sign_flip * lower_half * sine_table, field_in[..., ROT:]], axis=-1)

def round_trip(values):
    return lax.optimization_barrier(values.astype(jnp.bfloat16)).astype(jnp.float32)

def reference(hidden_in, ln_gain, ln_bias, qkv_weight, qkv_bias, dense_weight, dense_bias, fc1_weight, fc1_bias, fc2_weight, fc2_bias, cotangent):
    seq_count = TOKENS // LEN
    seq_group = max([count for count in range(1, 5) if seq_count % count == 0])
    block_rows = seq_group * LEN
    block_count = seq_count // seq_group
    score_scale = 1.0 / math.sqrt(HD)
    w_qkv = qkv_weight.reshape(D, 3 * D)
    b_qkv = qkv_bias.astype(jnp.float32).reshape(3 * D)
    b_up = fc1_bias.astype(jnp.float32).reshape(FF)
    gain = ln_gain.astype(jnp.float32)
    shift = ln_bias.astype(jnp.float32)
    out_bias = dense_bias.astype(jnp.float32) + fc2_bias.astype(jnp.float32)
    cosine, sine_table = rotary_tables(block_rows)
    causal = jnp.arange(LEN)[:, None] >= jnp.arange(LEN)[None, :]
    shape_four = (seq_group, LEN, H, HD)

    def step(carry, pair):
        tokens, grad_rows = pair
        x_full = tokens.astype(jnp.float32)
        average = lax.optimization_barrier(jnp.mean(x_full, axis=-1, keepdims=True))
        centred = x_full - average
        inv_std = lax.rsqrt(lax.optimization_barrier(jnp.mean(centred * centred, axis=-1, keepdims=True)) + EPSILON)
        x_hat = centred * inv_std
        normed = (x_hat * gain + shift).astype(jnp.bfloat16)
        qkv = (jnp.dot(normed, w_qkv, preferred_element_type=jnp.float32) + b_qkv).reshape(block_rows, 3, H, HD)
        q_full = round_trip(rotate(qkv[:, 0], cosine, sine_table, 1.0)).reshape(shape_four)
        k_full = round_trip(rotate(qkv[:, 1], cosine, sine_table, 1.0)).reshape(shape_four)
        v_full = round_trip(qkv[:, 2]).reshape(shape_four)
        scores = jnp.einsum('sqhd,skhd->shqk', q_full, k_full) * score_scale
        scores = jnp.where(causal, scores, -jnp.inf)
        row_peak = lax.optimization_barrier(jnp.max(scores, axis=-1, keepdims=True))
        log_total = row_peak + jnp.log(lax.optimization_barrier(jnp.sum(jnp.exp(scores - row_peak), axis=-1, keepdims=True)))
        probs_full = jnp.exp(scores - log_total)
        probs_round = round_trip(probs_full)
        context = jnp.einsum('shqk,skhd->sqhd', probs_round, v_full).astype(jnp.bfloat16).reshape(block_rows, D)
        hidden_pre = jnp.dot(normed, fc1_weight, preferred_element_type=jnp.float32) + b_up
        gelu_value, gelu_slope = gelu_pair(hidden_pre)
        act_rows = gelu_value.astype(jnp.bfloat16)
        branch = jnp.dot(context, dense_weight, preferred_element_type=jnp.float32) + jnp.dot(act_rows, fc2_weight, preferred_element_type=jnp.float32)
        out_rows = (x_full + branch + out_bias).astype(jnp.bfloat16)
        grad_full = grad_rows.astype(jnp.float32)
        fc2_term = jnp.dot(act_rows.T, grad_rows, preferred_element_type=jnp.float32)
        act_grad = jnp.dot(grad_rows, fc2_weight.T, preferred_element_type=jnp.float32)
        hidden_grad = act_grad * gelu_slope
        hidden_grad_b = hidden_grad.astype(jnp.bfloat16)
        fc1_bias_term = lax.optimization_barrier(jnp.sum(hidden_grad, axis=0))
        fc1_term = jnp.dot(normed.T, hidden_grad_b, preferred_element_type=jnp.float32)
        dense_term = jnp.dot(context.T, grad_rows, preferred_element_type=jnp.float32)
        context_grad = round_trip(jnp.dot(grad_rows, dense_weight.T, preferred_element_type=jnp.float32)).reshape(shape_four)
        prob_grad = jnp.einsum('sqhd,skhd->shqk', context_grad, v_full)
        row_delta = lax.optimization_barrier(jnp.sum(probs_full * prob_grad, axis=-1, keepdims=True))
        score_grad = round_trip(probs_full * (prob_grad - row_delta) * score_scale)
        query_grad = jnp.einsum('shqk,skhd->sqhd', score_grad, k_full).reshape(block_rows, H, HD)
        key_grad = jnp.einsum('shqk,sqhd->skhd', score_grad, q_full).reshape(block_rows, H, HD)
        value_grad = jnp.einsum('shqk,sqhd->skhd', probs_round, context_grad).reshape(block_rows, H, HD)
        qkv_grad = jnp.stack([rotate(query_grad, cosine, sine_table, -1.0), rotate(key_grad, cosine, sine_table, -1.0), value_grad], axis=1)
        qkv_bias_term = lax.optimization_barrier(jnp.sum(qkv_grad, axis=0))
        qkv_grad_b = qkv_grad.astype(jnp.bfloat16).reshape(block_rows, 3 * D)
        qkv_term = jnp.dot(normed.T, qkv_grad_b, preferred_element_type=jnp.float32)
        normed_grad = jnp.dot(hidden_grad_b, fc1_weight.T, preferred_element_type=jnp.float32) + jnp.dot(qkv_grad_b, w_qkv.T, preferred_element_type=jnp.float32)
        gain_term = lax.optimization_barrier(jnp.sum(normed_grad * x_hat, axis=0))
        shift_term = lax.optimization_barrier(jnp.sum(normed_grad, axis=0))
        grad_hat = normed_grad * gain
        input_rows = grad_full + inv_std * (grad_hat - lax.optimization_barrier(jnp.mean(grad_hat, axis=-1, keepdims=True)) - x_hat * lax.optimization_barrier(jnp.mean(grad_hat * x_hat, axis=-1, keepdims=True)))
        terms = (qkv_term, qkv_bias_term, dense_term, lax.optimization_barrier(jnp.sum(grad_full, axis=0)), fc1_term, fc1_bias_term, fc2_term, gain_term, shift_term)
        carry = jax.tree.map(lambda left, right: left + right, carry, terms)
        return (carry, (out_rows, input_rows))
    initial = (jnp.zeros((D, 3 * D), jnp.float32), jnp.zeros((3, H, HD), jnp.float32), jnp.zeros((D, D), jnp.float32), jnp.zeros((D,), jnp.float32), jnp.zeros((D, FF), jnp.float32), jnp.zeros((FF,), jnp.float32), jnp.zeros((FF, D), jnp.float32), jnp.zeros((D,), jnp.float32), jnp.zeros((D,), jnp.float32))
    x_blocks = hidden_in.reshape(block_count, block_rows, D)
    grad_blocks = cotangent.reshape(block_count, block_rows, D)
    final, (out_all, input_all) = lax.scan(step, initial, (x_blocks, grad_blocks))
    return (out_all.reshape(TOKENS, D), input_all.reshape(TOKENS, D), final[0].reshape(D, 3, D), final[1], final[2], final[3], final[4], final[5].reshape(FF // HD, HD), final[6], final[3], final[7], final[8])
```

```python
import functools
import math

import jax
import jax.numpy as jnp
import numpy as np
from jax import lax
from jax.experimental import pallas as pl
from jax.experimental.pallas import tpu as pltpu
from jax.sharding import PartitionSpec as P

HD = 64
ROT = 32
LEN = 512
EPSILON = 1e-05
GELU_C = math.sqrt(2.0 / math.pi)
F32 = jnp.float32
BF16 = jnp.bfloat16
ANY = pl.BlockSpec(memory_space=pl.ANY)
VMEM = pl.BlockSpec(memory_space=pltpu.VMEM)


def gelu_pair(h):
    square = h * h
    tangent = jnp.tanh(h * (GELU_C + (GELU_C * 0.044715) * square))
    half = 0.5 + 0.5 * tangent
    slope = half + 0.5 * h * (1.0 - tangent * tangent) * (GELU_C + (3.0 * 0.044715 * GELU_C) * square)
    return h * half, slope


def rotary_rows():
    position = np.arange(LEN, dtype=np.float32)
    frequency = (10000.0 ** (-np.arange(0, ROT, 2, dtype=np.float32) / ROT)).astype(np.float32)
    angles = (position[:, None] * frequency[None, :]).astype(np.float32)
    cosine, sine = np.cos(angles).astype(np.float32), np.sin(angles).astype(np.float32)
    rest = np.ones((LEN, HD - ROT), np.float32)
    none = np.zeros((LEN, ROT // 2), np.float32)
    here = np.concatenate([cosine, cosine, rest], axis=1)
    above = np.concatenate([-sine, none, 0 * rest], axis=1)
    below = np.concatenate([none, sine, 0 * rest], axis=1)
    return tuple(np.tile(part, (1, 2)) for part in (here, above, below))


def flip(index, mask):
    result, place = index, 1
    while place <= mask:
        if mask & place:
            result = result + (1 - 2 * ((index // place) % 2)) * place
        place *= 2
    return result


def span(bits):
    masks = [0]
    for bit in bits:
        masks = masks + [mask | (1 << bit) for mask in masks]
    return masks


def dot(a, b, dims):
    return lax.dot_general(a, b, (dims, ((), ())), preferred_element_type=F32)


NN, NT, TN = ((1,), (0,)), ((1,), (1,)), ((0,), (0,))


class Sizes:
    def __init__(self, groups, tensor, unit, width, hidden, heads_width):
        self.n, self.nt = groups, tensor
        self.bits = groups.bit_length() - 1
        self.unit, self.d, self.f, self.c = unit, width, hidden, heads_width
        self.rows = unit * tensor
        self.seqs = self.rows // LEN
        self.shard = width // groups
        self.q3 = 3 * heads_width
        self.n1 = self.q3 + hidden
        self.n2 = hidden + heads_width
        self.orders = (
            list(range(1, self.bits)) + [0],
            list(range(self.bits - 1, 0, -1)) + [0],
        )


def pack_rows(z):
    lanes = min(128, z.shard)
    per = z.shard // lanes
    return lanes, per, 4 * per, z.f // 128, z.q3 // 128


def rotated(tile, here, above, below):
    width = tile.shape[1]
    up = pltpu.roll(tile, width - ROT // 2, axis=1)
    down = pltpu.roll(tile, ROT // 2, axis=1)
    repeat = width // 128
    return (
        tile * jnp.tile(here, (1, repeat))
        + up * jnp.tile(above, (1, repeat))
        + down * jnp.tile(below, (1, repeat))
    )


def forward_kernel(z, compute, *refs):
    (x_hbm, c_hbm, wq_hbm, wu_hbm, wd_hbm, pack_hbm, t_here, t_above, t_below,
     normed_o, xhat_o, cot_o, qkv_o, act_o, hg_o, ctx_o, dctx_o, branch_o, w1_o, small_o,
     w, xs, xh, cs, qkv, act, hg, ctx, dctx, nm, slots, vec, bias, small,
     loc_sem, out_sem, pk_send, pk_recv, w_send, w_recv, z_send, z_recv) = refs
    n, nt, R = z.n, z.nt, z.unit
    me, t = lax.axis_index("dp"), lax.axis_index("tensor")

    barrier = pltpu.get_barrier_semaphore()
    for m in range(1, n):
        pl.semaphore_signal(barrier, inc=1, device_id={"dp": flip(me, m)}, device_id_type=pl.DeviceIdType.MESH)
    for step in (1, nt - 1):
        pl.semaphore_signal(barrier, inc=1, device_id={"tensor": lax.rem(t + step, nt)}, device_id_type=pl.DeviceIdType.MESH)
    pl.semaphore_wait(barrier, n - 1 + 2)

    waits = []

    def remote(src, dst, send, recv, where):
        return pltpu.make_async_remote_copy(
            src_ref=src, dst_ref=dst, send_sem=send, recv_sem=recv, device_id=where, device_id_type=pl.DeviceIdType.MESH
        )

    def pack_copy(m, receive):
        slot = slots.at[flip(me, m)] if receive else slots.at[me]
        return remote(pack_hbm, slot, pk_send.at[m], pk_recv.at[m], {"dp": flip(me, m)})

    for m in range(1, n):
        copy = pack_copy(m, False)
        copy.start()
        waits.append((None, copy))
    own_pack = pltpu.make_async_copy(pack_hbm, slots.at[me], loc_sem.at[0])
    own_pack.start()

    def rows_of(u):
        return pl.ds(pl.multiple_of(u * R, R), R)

    def line(buf, which, j, up, receive):
        src = (t - (j - 1)) if up else (t + (j - 1))
        got = (t - j) if up else (t + j)
        unit = got if receive else src
        to = (t + 1) if up else (t - 1)
        ref = buf.at[rows_of(unit), :]
        s = (which * 2 + (0 if up else 1)) * nt + j
        return remote(ref, ref, z_send.at[s], z_recv.at[s], {"tensor": to})

    def sends(j, up):
        return ((t < nt - 1) & (t >= j - 1)) if up else ((t > 0) & (t <= nt - j))

    def gets(j, up):
        return (t >= j) if up else (t <= nt - 1 - j)

    def line_send(buf, which, j, up, extra=None):
        cond = sends(j, up) if extra is None else sends(j, up) & extra

        @pl.when(cond)
        def _():
            line(buf, which, j, up, False).start()

    def line_recv(buf, which, j, up):
        @pl.when(gets(j, up))
        def _():
            line(buf, which, j, up, True).wait_recv()

    def line_sent(buf, which):
        for j in range(1, nt):
            for up in (True, False):
                @pl.when(sends(j, up))
                def _():
                    line(buf, which, j, up, False).wait_send()

    own_x = pltpu.make_async_copy(x_hbm, xs.at[rows_of(t), :], loc_sem.at[1])
    own_x.start()
    own_c = pltpu.make_async_copy(c_hbm, cs.at[rows_of(t), :], loc_sem.at[2])
    own_c.start()

    chunks = [(wq_hbm, 0, z.q3), (wu_hbm, z.q3, z.f), (wd_hbm, z.n1, z.n2)]

    def slot_ref(d, col, width):
        return w.at[pl.ds(pl.multiple_of(d * z.shard, z.shard), z.shard), pl.ds(col, width)]

    def w_copy(c, h, stage, m, receive):
        src_hbm, col, width = chunks[c]
        half = width // 2
        col = col + h * half
        bit = z.orders[h][stage]
        to = flip(me, 1 << bit)
        d = flip(me, m | (1 << bit)) if receive else flip(me, m)
        dst = slot_ref(d, col, half)
        src = dst
        if m == 0 and not receive:
            src = src_hbm.at[:, pl.ds(h * half, half)]
        s = (c * 2 + h) * n + (m | (1 << bit))
        return remote(src, dst, w_send.at[s], w_recv.at[s], {"dp": to})

    def w_start(c, stage):
        for h in (0, 1):
            for m in span(z.orders[h][:stage]):
                copy = w_copy(c, h, stage, m, False)
                copy.start()
                waits.append((None, copy))

    def w_wait(c, stage):
        for h in (0, 1):
            for m in span(z.orders[h][:stage]):
                w_copy(c, h, stage, m, True).wait_recv()

    for c, (src, col, width) in enumerate(chunks):
        pltpu.make_async_copy(src, slot_ref(me, col, width), loc_sem.at[3 + c]).start()

    w_start(0, 0)
    own_x.wait()
    line_send(xs, 0, 1, True)
    line_send(xs, 0, 1, False)
    w_start(1, 0)
    own_c.wait()

    def cot_starts(j):
        line_send(cs, 1, 1, True, t == j)
        line_send(cs, 1, 1, False, t == nt - 1 - j)

    cot_starts(0)

    def x_event(j):
        for up in (True, False):
            line_recv(xs, 0, j, up)
        if j < nt - 1:
            for up in (True, False):
                line_send(xs, 0, j + 1, up)
        cot_starts(j)

    def c_event(j):
        for up in (True, False):
            line_recv(cs, 1, j, up)
        if j < nt - 1:
            for up in (True, False):
                line_send(cs, 1, j + 1, up)

    for m in range(1, n):
        pack_copy(m, True).wait_recv()
    own_pack.wait()
    for c, (src, col, width) in enumerate(chunks):
        pltpu.make_async_copy(src, slot_ref(me, col, width), loc_sem.at[3 + c]).wait()

    outs = []

    def put(src, dst):
        copy = pltpu.make_async_copy(src, dst, out_sem.at[len(outs)])
        copy.start()
        outs.append(copy)

    last = z.bits - 1

    lanes, per, base, frows, qrows = pack_rows(z)

    def vectors():
        for v in range(4):
            for d in range(n):
                for r in range(per):
                    at = d * z.shard + r * lanes
                    vec[pl.ds(v, 1), pl.ds(at, lanes)] = slots[d, pl.ds(v * per + r, 1), :lanes].astype(F32)
        total = jnp.zeros((frows + qrows, 128), F32)
        for d in range(n):
            total = total + slots[d, pl.ds(base, frows + qrows), :].astype(F32)
        for r in range(qrows):
            bias[:, pl.ds(r * 128, 128)] = total[frows + r:frows + r + 1, :]
        for r in range(frows):
            bias[:, pl.ds(z.q3 + r * 128, 128)] = total[r:r + 1, :]

    def layer_norm(seq):
        block = 16

        def body(i, _):
            rows = pl.ds(pl.multiple_of(seq * LEN + i * block, block), block)
            full = xs[rows, :].astype(F32)
            centred = full - jnp.mean(full, axis=1, keepdims=True)
            inv_std = lax.rsqrt(jnp.mean(centred * centred, axis=1, keepdims=True) + EPSILON)
            hat = centred * inv_std
            xh[rows, :] = hat.astype(BF16)
            nm[rows, :] = (hat * vec[0:1, :] + vec[1:2, :]).astype(BF16)
            return 0

        lax.fori_loop(0, LEN // block, body, 0)

    def seq_rows(seq):
        return pl.ds(pl.multiple_of(seq * LEN, LEN), LEN)

    def qkv_tiles(seq):
        rows = seq_rows(seq)
        for part in range(3):
            cols = pl.ds(part * z.c, z.c)
            tile = dot(nm[rows, :], w[:, cols], NN) + bias[:, cols]
            if part < 2:
                tile = rotated(tile, t_here[...], t_above[...], t_below[...])
            qkv[rows, cols] = tile.astype(BF16)

    def up_tiles(seq, first, count):
        rows = seq_rows(seq)

        def body(j, _):
            cols = pl.ds(pl.multiple_of(j * 512, 512), 512)
            wcols = pl.ds(pl.multiple_of(z.q3 + j * 512, 512), 512)
            tile = dot(nm[rows, :], w[:, wcols], NN) + bias[:, wcols]
            value, slope = gelu_pair(tile)
            act[rows, cols] = value.astype(BF16)
            hg[rows, cols] = slope.astype(BF16)
            return 0

        lax.fori_loop(first, first + count, body, 0)

    half_rows = LEN // 2

    def attend(seq):
        low = lax.broadcasted_iota(jnp.int32, (half_rows, 128), 1) < HD

        def pair(p, _):
            def block(part, start, count):
                cols = pl.ds(pl.multiple_of(part * z.c + p * 128, 128), 128)
                return qkv[pl.ds(pl.multiple_of(seq * LEN + start, half_rows), count), cols]

            for qb in range(2):
                keys = half_rows * (qb + 1)
                q2 = block(0, qb * half_rows, half_rows) * BF16(0.125)
                k2 = block(1, 0, keys)
                v2 = block(2, 0, keys)
                row = lax.broadcasted_iota(jnp.int32, (half_rows, keys), 0) + qb * half_rows
                seen = lax.broadcasted_iota(jnp.int32, (half_rows, keys), 1) <= row
                parts = []
                for side in range(2):
                    q1 = jnp.where(low if side == 0 else ~low, q2, BF16(0))
                    scores = jnp.where(seen, dot(q1, k2, NT), -1e30)
                    peak = jnp.max(scores, axis=1, keepdims=True)
                    e = jnp.exp(scores - peak)
                    prob = e * (1.0 / jnp.sum(e, axis=1, keepdims=True))
                    parts.append(dot(prob.astype(BF16), v2, NN))
                out = jnp.where(low, parts[0], parts[1]).astype(BF16)
                ctx[pl.ds(pl.multiple_of(seq * LEN + qb * half_rows, half_rows), half_rows),
                    pl.ds(pl.multiple_of(p * 128, 128), 128)] = out
            return 0

        lax.fori_loop(0, z.c // 128, pair, 0)

    def branch_tiles(seq):
        rows = seq_rows(seq)

        def body(j, _):
            wrows = pl.ds(pl.multiple_of(j * 512, 512), 512)
            tile = dot(act[rows, :], w[wrows, pl.ds(z.n1, z.f)], NT)
            tile = tile + dot(ctx[rows, :], w[wrows, pl.ds(z.n1 + z.f, z.c)], NT)
            xs[rows, wrows] = tile.astype(BF16)
            return 0

        lax.fori_loop(0, z.d // 512, body, 0)

    def grad_tiles(seq):
        rows = seq_rows(seq)

        def body(j, _):
            cols = pl.ds(pl.multiple_of(j * 512, 512), 512)
            wcols = pl.ds(pl.multiple_of(z.n1 + j * 512, 512), 512)
            grad = dot(cs[rows, :], w[:, wcols], NN) * hg[rows, cols].astype(F32)
            small[1:2, cols] += jnp.sum(grad, axis=0, keepdims=True)
            hg[rows, cols] = grad.astype(BF16)
            return 0

        lax.fori_loop(0, z.f // 512, body, 0)
        dctx[rows, :] = dot(cs[rows, :], w[:, pl.ds(z.n1 + z.f, z.c)], NN).astype(BF16)

        def sums(i, _):
            part = cs[pl.ds(pl.multiple_of(seq * LEN + i * 64, 64), 64), :].astype(F32)
            small[0:1, :] += jnp.sum(part, axis=0, keepdims=True)
            return 0

        lax.fori_loop(0, LEN // 64, sums, 0)

    mine = t // (nt // z.seqs)
    other = z.seqs - 1 - mine
    if not compute:
        x_event(1)
        w_wait(0, 0); w_start(0, 1); w_start(2, 0)
        w_wait(1, 0); w_wait(0, 1); w_start(1, 1); w_start(0, 2)
        x_event(2)
        w_wait(2, 0); w_wait(1, 1); w_start(2, 1); w_start(1, 2)
        x_event(3)
        w_wait(0, 2); w_wait(1, 2); w_wait(2, 1); w_start(2, 2)
        c_event(1)
        w_wait(2, 2)
        c_event(2)
        c_event(3)
    else:
        small[...] = jnp.zeros_like(small)
        vectors()
        w_wait(0, 0); w_start(0, 1); w_start(2, 0)
        x_event(1)
        layer_norm(mine)
        w_wait(1, 0); w_wait(0, 1); w_start(1, 1); w_start(0, 2)
        w_wait(0, 2)
        qkv_tiles(mine)
        x_event(2)
        attend(mine)
        w_wait(2, 0); w_wait(1, 1); w_start(2, 1); w_start(1, 2)
        x_event(3)
        layer_norm(other)
        put(nm, normed_o); put(xh, xhat_o)
        qkv_tiles(other)
        put(qkv, qkv_o)
        w_wait(1, 2)
        put(w.at[:, pl.ds(0, z.n1)], w1_o)
        up_tiles(mine, 0, z.f // 512)
        c_event(1)
        w_wait(2, 1); w_start(2, 2)
        up_tiles(other, 0, z.f // 512)
        put(act, act_o)
        attend(other)
        put(ctx, ctx_o)
        w_wait(2, 2)
        line_sent(xs, 0)
        branch_tiles(mine)
        c_event(2)
        branch_tiles(other)
        put(xs, branch_o)
        grad_tiles(mine)
        c_event(3)
        put(cs, cot_o)
        grad_tiles(other)
        small[2:3, :z.d] = vec[0:1, :]
        small[3:4, :z.d] = vec[2:3, :] + vec[3:4, :]
        put(hg, hg_o); put(dctx, dctx_o); put(small, small_o)

    for cond, copy in waits:
        copy.wait_send()
    line_sent(cs, 1)
    if not compute:
        line_sent(xs, 0)
        put(xs, normed_o); put(xs, xhat_o); put(cs, cot_o); put(w.at[:, pl.ds(0, z.n1)], w1_o)
    for copy in outs:
        copy.wait()


def packed(z, ln_gain, ln_bias, dense_bias, fc2_bias, fc1_bias, qkv_bias):
    lanes, per, base, frows, qrows = pack_rows(z)
    me = lax.axis_index("dp")
    mine = jnp.arange(z.n)[None, :, None] == me
    def spread(a):
        rows, cols = a.reshape(-1, a.shape[-1]).shape
        return jnp.where(mine, a.reshape(rows, 1, cols), BF16(0)).reshape(-1, 128)
    plain = jnp.concatenate([v.reshape(per, lanes) for v in (ln_gain, ln_bias, dense_bias, fc2_bias)], axis=0)
    if lanes < 128:
        plain = jnp.pad(plain, ((0, 0), (0, 128 - lanes)))
    rows = jnp.concatenate([plain, spread(fc1_bias), spread(qkv_bias)], axis=0)
    return jnp.pad(rows, ((0, -rows.shape[0] % 16), (0, 0)))


def forward(z, compute, x, cot, wq, wu, wd, pack):
    prows = pack.shape[0]
    shape = lambda s, dt=BF16: jax.ShapeDtypeStruct(s, dt)
    T = z.rows
    outs = [shape((T, z.d)), shape((T, z.d)), shape((T, z.d)), shape((T, z.q3)), shape((T, z.f)), shape((T, z.f)),
            shape((T, z.c)), shape((T, z.c)), shape((T, z.d)), shape((z.d, z.n1)), shape((8, max(z.d, z.f)), F32)]
    v = pltpu.VMEM
    sem = pltpu.SemaphoreType.DMA
    scratch = [v((z.d, z.n1 + z.n2), BF16), v((T, z.d), BF16), v((T, z.d), BF16), v((T, z.d), BF16), v((T, z.q3), BF16),
               v((T, z.f), BF16), v((T, z.f), BF16), v((T, z.c), BF16), v((T, z.c), BF16), v((T, z.d), BF16),
               v((z.n, prows, 128), BF16), v((8, z.d), F32), v((1, z.n1), F32), v((8, max(z.d, z.f)), F32),
               sem((6,)), sem((12,)), sem((z.n,)), sem((z.n,)), sem((6 * z.n,)), sem((6 * z.n,)), sem((4 * z.nt,)), sem((4 * z.nt,))]
    return pl.pallas_call(
        functools.partial(forward_kernel, z, compute),
        out_shape=outs,
        in_specs=[ANY] * 6 + [VMEM] * 3,
        out_specs=[ANY] * len(outs),
        scratch_shapes=scratch,
        compiler_params=pltpu.CompilerParams(collective_id=0, has_side_effects=True, vmem_limit_bytes=67_043_328),
        name="forward_kernel",
    )(x, cot, wq, wu, wd, pack, *(jnp.asarray(p) for p in rotary_rows()))


def attention_backward(z, qkv, dctx):
    heads = z.c // HD
    four = (z.seqs, LEN, heads, HD)
    q, k, v = (qkv[:, i * z.c:(i + 1) * z.c].reshape(four) for i in range(3))
    g = dctx.reshape(four)
    seen = jnp.arange(LEN)[:, None] >= jnp.arange(LEN)[None, :]
    scores = jnp.einsum("sqhd,skhd->shqk", q, k, preferred_element_type=F32) * 0.125
    probs = jax.nn.softmax(jnp.where(seen, scores, -jnp.inf), axis=-1)
    grad = jnp.einsum("sqhd,skhd->shqk", g, v, preferred_element_type=F32)
    delta = jnp.sum(probs * grad, axis=-1, keepdims=True)
    ds = (probs * (grad - delta) * 0.125).astype(BF16)
    dq = jnp.einsum("shqk,skhd->sqhd", ds, k, preferred_element_type=F32)
    dk = jnp.einsum("shqk,sqhd->skhd", ds, q, preferred_element_type=F32)
    dv = jnp.einsum("shqk,sqhd->skhd", probs.astype(BF16), g, preferred_element_type=F32)
    here, above, below = (jnp.tile(jnp.asarray(p)[:, :HD], (z.seqs, 1)).reshape(z.seqs, LEN, 1, HD) for p in rotary_rows())
    def back(a):
        return a * here + jnp.roll(a * above, ROT // 2, axis=-1) + jnp.roll(a * below, -(ROT // 2), axis=-1)
    return jnp.concatenate([a.reshape(z.rows, z.c) for a in (back(dq), back(dk), dv)], axis=1)


def shards(x, ln_gain, ln_bias, qkv_weight, qkv_bias, dense_weight, dense_bias, fc1_weight, fc1_bias, fc2_weight, fc2_bias, cotangent):
    z = Sizes(lax.axis_size("dp"), lax.axis_size("tensor"), x.shape[0], x.shape[1], fc1_weight.shape[1], dense_weight.shape[0])
    pack = packed(z, ln_gain, ln_bias, dense_bias, fc2_bias, fc1_bias, qkv_bias)
    wd = jnp.concatenate([fc2_weight.T, dense_weight.T], axis=1)
    normed, xhat, cot, qkv, act, hg, ctx, dctx, branch, w1, small = forward(
        z, True, x, cotangent, qkv_weight.reshape(z.shard, z.q3), fc1_weight, wd, pack)
    scatter = lambda a, axis, dim: lax.psum_scatter(a, axis, scatter_dimension=dim, tiled=True)
    xf = x.astype(F32)
    centred = xf - jnp.mean(xf, axis=-1, keepdims=True)
    inv_std = lax.rsqrt(jnp.mean(centred * centred, axis=-1, keepdims=True) + EPSILON)
    hat = centred * inv_std
    gain = small[2:3, :z.d]
    hidden_out = (xf + scatter(branch, "tensor", 0).astype(F32) + small[3:4, :z.d]).astype(BF16)
    dqkv = attention_backward(z, qkv, dctx)
    dqkv_b = dqkv.astype(BF16)
    left = jnp.concatenate([dqkv_b, hg], axis=1)
    ngrad = jnp.dot(left, w1.T, preferred_element_type=F32)
    nl = scatter(ngrad.astype(BF16), "tensor", 0).astype(F32)
    gh = nl * gain
    input_grad = cotangent.astype(F32) + inv_std * (gh - jnp.mean(gh, -1, keepdims=True) - hat * jnp.mean(gh * hat, -1, keepdims=True))
    dw = lambda a, b: jnp.einsum("rd,rc->dc", a, b, preferred_element_type=F32).astype(BF16)
    d1 = scatter(dw(normed, left), "dp", 0).astype(F32)
    d2 = scatter(dw(cot, jnp.concatenate([act, ctx], axis=1)), "dp", 0).astype(F32)
    vecs = lax.psum(jnp.concatenate([small[0], small[1, :z.f], jnp.sum(dqkv, axis=0)]), "dp")
    lnv = lax.psum(jnp.stack([jnp.sum(nl * hat, axis=0), jnp.sum(nl, axis=0)]), ("dp", "tensor"))
    i, t = lax.axis_index("dp"), lax.axis_index("tensor")
    part = z.d // (z.n * z.nt)
    cut = lambda a: lax.dynamic_slice_in_dim(a, (i * z.nt + t) * part, part, 0)
    hc = HD // z.n
    dbias = cut(vecs[:z.d])
    fb = lax.dynamic_slice_in_dim(vecs[z.d:z.d + z.f].reshape(-1, HD), i * hc, hc, 1)
    qb = lax.dynamic_slice_in_dim(vecs[z.d + z.f:].reshape(3, -1, HD), i * hc, hc, 2)
    return (hidden_out, input_grad, d1[:, :z.q3].reshape(z.shard, 3, z.c), qb, d2[:, z.f:].T, dbias, d1[:, z.q3:], fb, d2[:, :z.f].T, dbias,
            cut(lnv[0]), cut(lnv[1]))


def solution(mesh):
    both = ("dp", "tensor")
    placed = (
        P(both, None), P("dp"), P("dp"), P("dp", None, "tensor"), P(None, "tensor", "dp"), P("tensor", "dp"),
        P("dp"), P("dp", "tensor"), P("tensor", "dp"), P("tensor", "dp"), P("dp"), P(both, None),
    )
    given = (
        P(both, None), P(both, None), P("dp", None, "tensor"), P(None, "tensor", "dp"), P("tensor", "dp"), P(both),
        P("dp", "tensor"), P("tensor", "dp"), P("tensor", "dp"), P(both), P(both), P(both),
    )
    return jax.shard_map(shards, mesh=mesh, in_specs=placed, out_specs=given, check_vma=False)
```

```python
import functools
import math

import jax
import jax.numpy as jnp
import numpy as np
from jax import lax
from jax.experimental import pallas as pl
from jax.experimental.pallas import tpu as pltpu
from jax.sharding import PartitionSpec as P

HD = 64
ROT = 32
LEN = 512
EPSILON = 1e-05
GELU_C = math.sqrt(2.0 / math.pi)
F32 = jnp.float32
BF16 = jnp.bfloat16
ANY = pl.BlockSpec(memory_space=pl.ANY)
VMEM = pl.BlockSpec(memory_space=pltpu.VMEM)


def gelu_pair(h):
    square = h * h
    tangent = jnp.tanh(h * (GELU_C + (GELU_C * 0.044715) * square))
    half = 0.5 + 0.5 * tangent
    slope = half + 0.5 * h * (1.0 - tangent * tangent) * (GELU_C + (3.0 * 0.044715 * GELU_C) * square)
    return h * half, slope


def rotary_rows():
    position = np.arange(LEN, dtype=np.float32)
    frequency = (10000.0 ** (-np.arange(0, ROT, 2, dtype=np.float32) / ROT)).astype(np.float32)
    angles = (position[:, None] * frequency[None, :]).astype(np.float32)
    cosine, sine = np.cos(angles).astype(np.float32), np.sin(angles).astype(np.float32)
    rest = np.ones((LEN, HD - ROT), np.float32)
    none = np.zeros((LEN, ROT // 2), np.float32)
    here = np.concatenate([cosine, cosine, rest], axis=1)
    above = np.concatenate([-sine, none, 0 * rest], axis=1)
    below = np.concatenate([none, sine, 0 * rest], axis=1)
    return tuple(np.tile(part, (1, 2)) for part in (here, above, below))


def flip(index, mask):
    result, place = index, 1
    while place <= mask:
        if mask & place:
            result = result + (1 - 2 * ((index // place) % 2)) * place
        place *= 2
    return result


def span(bits):
    masks = [0]
    for bit in bits:
        masks = masks + [mask | (1 << bit) for mask in masks]
    return masks


def dot(a, b, dims):
    return lax.dot_general(a, b, (dims, ((), ())), preferred_element_type=F32)


NN, NT, TN = ((1,), (0,)), ((1,), (1,)), ((0,), (0,))


class Sizes:
    def __init__(self, groups, tensor, unit, width, hidden, heads_width):
        self.n, self.nt = groups, tensor
        self.bits = groups.bit_length() - 1
        self.unit, self.d, self.f, self.c = unit, width, hidden, heads_width
        self.rows = unit * tensor
        self.seqs = self.rows // LEN
        self.shard = width // groups
        self.q3 = 3 * heads_width
        self.n1 = self.q3 + hidden
        self.n2 = hidden + heads_width
        self.orders = (
            list(range(1, self.bits)) + [0],
            list(range(self.bits - 1, 0, -1)) + [0],
        )
        self.orders_back = tuple(list(reversed(order)) for order in self.orders)


def pack_rows(z):
    lanes = min(128, z.shard)
    per = z.shard // lanes
    return lanes, per, 4 * per, z.f // 128, z.q3 // 128


def rotated(tile, here, above, below):
    width = tile.shape[1]
    up = pltpu.roll(tile, width - ROT // 2, axis=1)
    down = pltpu.roll(tile, ROT // 2, axis=1)
    repeat = width // 128
    return (
        tile * jnp.tile(here, (1, repeat))
        + up * jnp.tile(above, (1, repeat))
        + down * jnp.tile(below, (1, repeat))
    )


def forward_kernel(z, compute, *refs):
    (x_hbm, c_hbm, wq_hbm, wu_hbm, wd_hbm, pack_hbm, t_here, t_above, t_below,
     normed_o, xhat_o, cot_o, qkv_o, act_o, hg_o, ctx_o, dctx_o, branch_o, w1_o, small_o,
     w, xs, xh, cs, qkv, act, hg, ctx, dctx, nm, slots, vec, bias, small,
     loc_sem, out_sem, pk_send, pk_recv, w_send, w_recv, z_send, z_recv) = refs
    n, nt, R = z.n, z.nt, z.unit
    me, t = lax.axis_index("dp"), lax.axis_index("tensor")

    barrier = pltpu.get_barrier_semaphore()
    for m in range(1, n):
        pl.semaphore_signal(barrier, inc=1, device_id={"dp": flip(me, m)}, device_id_type=pl.DeviceIdType.MESH)
    for step in (1, nt - 1):
        pl.semaphore_signal(barrier, inc=1, device_id={"tensor": lax.rem(t + step, nt)}, device_id_type=pl.DeviceIdType.MESH)
    pl.semaphore_wait(barrier, n - 1 + 2)

    waits = []

    def remote(src, dst, send, recv, where):
        return pltpu.make_async_remote_copy(
            src_ref=src, dst_ref=dst, send_sem=send, recv_sem=recv, device_id=where, device_id_type=pl.DeviceIdType.MESH
        )

    def pack_copy(m, receive):
        slot = slots.at[flip(me, m)] if receive else slots.at[me]
        return remote(pack_hbm, slot, pk_send.at[m], pk_recv.at[m], {"dp": flip(me, m)})

    for m in range(1, n):
        copy = pack_copy(m, False)
        copy.start()
        waits.append((None, copy))
    own_pack = pltpu.make_async_copy(pack_hbm, slots.at[me], loc_sem.at[0])
    own_pack.start()

    def rows_of(u):
        return pl.ds(pl.multiple_of(u * R, R), R)

    def line(buf, which, j, up, receive):
        src = (t - (j - 1)) if up else (t + (j - 1))
        got = (t - j) if up else (t + j)
        unit = got if receive else src
        to = (t + 1) if up else (t - 1)
        ref = buf.at[rows_of(unit), :]
        s = (which * 2 + (0 if up else 1)) * nt + j
        return remote(ref, ref, z_send.at[s], z_recv.at[s], {"tensor": to})

    def sends(j, up):
        return ((t < nt - 1) & (t >= j - 1)) if up else ((t > 0) & (t <= nt - j))

    def gets(j, up):
        return (t >= j) if up else (t <= nt - 1 - j)

    def line_send(buf, which, j, up, extra=None):
        cond = sends(j, up) if extra is None else sends(j, up) & extra

        @pl.when(cond)
        def _():
            line(buf, which, j, up, False).start()

    def line_recv(buf, which, j, up):
        @pl.when(gets(j, up))
        def _():
            line(buf, which, j, up, True).wait_recv()

    def line_sent(buf, which):
        for j in range(1, nt):
            for up in (True, False):
                @pl.when(sends(j, up))
                def _():
                    line(buf, which, j, up, False).wait_send()

    own_x = pltpu.make_async_copy(x_hbm, xs.at[rows_of(t), :], loc_sem.at[1])
    own_x.start()
    own_c = pltpu.make_async_copy(c_hbm, cs.at[rows_of(t), :], loc_sem.at[2])
    own_c.start()

    chunks = [(wq_hbm, 0, z.q3), (wu_hbm, z.q3, z.f), (wd_hbm, z.n1, z.n2)]

    def slot_ref(d, col, width):
        return w.at[pl.ds(pl.multiple_of(d * z.shard, z.shard), z.shard), pl.ds(col, width)]

    def w_copy(c, h, stage, m, receive):
        src_hbm, col, width = chunks[c]
        half = width // 2
        col = col + h * half
        bit = z.orders[h][stage]
        to = flip(me, 1 << bit)
        d = flip(me, m | (1 << bit)) if receive else flip(me, m)
        dst = slot_ref(d, col, half)
        src = dst
        if m == 0 and not receive:
            src = src_hbm.at[:, pl.ds(h * half, half)]
        s = (c * 2 + h) * n + (m | (1 << bit))
        return remote(src, dst, w_send.at[s], w_recv.at[s], {"dp": to})

    def w_start(c, stage):
        for h in (0, 1):
            for m in span(z.orders[h][:stage]):
                copy = w_copy(c, h, stage, m, False)
                copy.start()
                waits.append((None, copy))

    def w_wait(c, stage):
        for h in (0, 1):
            for m in span(z.orders[h][:stage]):
                w_copy(c, h, stage, m, True).wait_recv()

    for c, (src, col, width) in enumerate(chunks):
        pltpu.make_async_copy(src, slot_ref(me, col, width), loc_sem.at[3 + c]).start()

    w_start(0, 0)
    own_x.wait()
    line_send(xs, 0, 1, True)
    line_send(xs, 0, 1, False)
    w_start(1, 0)
    own_c.wait()

    def cot_starts(j):
        line_send(cs, 1, 1, True, t == j)
        line_send(cs, 1, 1, False, t == nt - 1 - j)

    cot_starts(0)

    def x_event(j):
        for up in (True, False):
            line_recv(xs, 0, j, up)
        if j < nt - 1:
            for up in (True, False):
                line_send(xs, 0, j + 1, up)
        cot_starts(j)

    def c_event(j):
        for up in (True, False):
            line_recv(cs, 1, j, up)
        if j < nt - 1:
            for up in (True, False):
                line_send(cs, 1, j + 1, up)

    for m in range(1, n):
        pack_copy(m, True).wait_recv()
    own_pack.wait()
    for c, (src, col, width) in enumerate(chunks):
        pltpu.make_async_copy(src, slot_ref(me, col, width), loc_sem.at[3 + c]).wait()

    outs = []

    def put(src, dst):
        copy = pltpu.make_async_copy(src, dst, out_sem.at[len(outs)])
        copy.start()
        outs.append(copy)

    last = z.bits - 1

    lanes, per, base, frows, qrows = pack_rows(z)

    def vectors():
        for v in range(4):
            for d in range(n):
                for r in range(per):
                    at = d * z.shard + r * lanes
                    vec[pl.ds(v, 1), pl.ds(at, lanes)] = slots[d, pl.ds(v * per + r, 1), :lanes].astype(F32)
        total = jnp.zeros((frows + qrows, 128), F32)
        for d in range(n):
            total = total + slots[d, pl.ds(base, frows + qrows), :].astype(F32)
        for r in range(qrows):
            bias[:, pl.ds(r * 128, 128)] = total[frows + r:frows + r + 1, :]
        for r in range(frows):
            bias[:, pl.ds(z.q3 + r * 128, 128)] = total[r:r + 1, :]

    def layer_norm(seq):
        block = 16

        def body(i, _):
            rows = pl.ds(pl.multiple_of(seq * LEN + i * block, block), block)
            full = xs[rows, :].astype(F32)
            centred = full - jnp.mean(full, axis=1, keepdims=True)
            inv_std = lax.rsqrt(jnp.mean(centred * centred, axis=1, keepdims=True) + EPSILON)
            hat = centred * inv_std
            xh[rows, :] = hat.astype(BF16)
            nm[rows, :] = (hat * vec[0:1, :] + vec[1:2, :]).astype(BF16)
            return 0

        lax.fori_loop(0, LEN // block, body, 0)

    def seq_rows(seq):
        return pl.ds(pl.multiple_of(seq * LEN, LEN), LEN)

    def qkv_tiles(seq):
        rows = seq_rows(seq)
        for part in range(3):
            cols = pl.ds(part * z.c, z.c)
            tile = dot(nm[rows, :], w[:, cols], NN) + bias[:, cols]
            if part < 2:
                tile = rotated(tile, t_here[...], t_above[...], t_below[...])
            qkv[rows, cols] = tile.astype(BF16)

    def up_tiles(seq, first, count):
        rows = seq_rows(seq)

        def body(j, _):
            cols = pl.ds(pl.multiple_of(j * 512, 512), 512)
            wcols = pl.ds(pl.multiple_of(z.q3 + j * 512, 512), 512)
            tile = dot(nm[rows, :], w[:, wcols], NN) + bias[:, wcols]
            value, slope = gelu_pair(tile)
            act[rows, cols] = value.astype(BF16)
            hg[rows, cols] = slope.astype(BF16)
            return 0

        lax.fori_loop(first, first + count, body, 0)

    half_rows = LEN // 2

    def attend(seq):
        low = lax.broadcasted_iota(jnp.int32, (half_rows, 128), 1) < HD

        def pair(p, _):
            def block(part, start, count):
                cols = pl.ds(pl.multiple_of(part * z.c + p * 128, 128), 128)
                return qkv[pl.ds(pl.multiple_of(seq * LEN + start, half_rows), count), cols]

            for qb in range(2):
                keys = half_rows * (qb + 1)
                q2 = block(0, qb * half_rows, half_rows) * BF16(0.125)
                k2 = block(1, 0, keys)
                v2 = block(2, 0, keys)
                row = lax.broadcasted_iota(jnp.int32, (half_rows, keys), 0) + qb * half_rows
                seen = lax.broadcasted_iota(jnp.int32, (half_rows, keys), 1) <= row
                parts = []
                for side in range(2):
                    q1 = jnp.where(low if side == 0 else ~low, q2, BF16(0))
                    scores = jnp.where(seen, dot(q1, k2, NT), -1e30)
                    peak = jnp.max(scores, axis=1, keepdims=True)
                    e = jnp.exp(scores - peak)
                    prob = e * (1.0 / jnp.sum(e, axis=1, keepdims=True))
                    parts.append(dot(prob.astype(BF16), v2, NN))
                out = jnp.where(low, parts[0], parts[1]).astype(BF16)
                ctx[pl.ds(pl.multiple_of(seq * LEN + qb * half_rows, half_rows), half_rows),
                    pl.ds(pl.multiple_of(p * 128, 128), 128)] = out
            return 0

        lax.fori_loop(0, z.c // 128, pair, 0)

    def branch_tiles(seq):
        rows = seq_rows(seq)

        def body(j, _):
            wrows = pl.ds(pl.multiple_of(j * 512, 512), 512)
            tile = dot(act[rows, :], w[wrows, pl.ds(z.n1, z.f)], NT)
            tile = tile + dot(ctx[rows, :], w[wrows, pl.ds(z.n1 + z.f, z.c)], NT)
            xs[rows, wrows] = tile.astype(BF16)
            return 0

        lax.fori_loop(0, z.d // 512, body, 0)

    def grad_tiles(seq):
        rows = seq_rows(seq)

        def body(j, _):
            cols = pl.ds(pl.multiple_of(j * 512, 512), 512)
            wcols = pl.ds(pl.multiple_of(z.n1 + j * 512, 512), 512)
            grad = dot(cs[rows, :], w[:, wcols], NN) * hg[rows, cols].astype(F32)
            small[1:2, cols] += jnp.sum(grad, axis=0, keepdims=True)
            hg[rows, cols] = grad.astype(BF16)
            return 0

        lax.fori_loop(0, z.f // 512, body, 0)
        dctx[rows, :] = dot(cs[rows, :], w[:, pl.ds(z.n1 + z.f, z.c)], NN).astype(BF16)

        def sums(i, _):
            part = cs[pl.ds(pl.multiple_of(seq * LEN + i * 64, 64), 64), :].astype(F32)
            small[0:1, :] += jnp.sum(part, axis=0, keepdims=True)
            return 0

        lax.fori_loop(0, LEN // 64, sums, 0)

    mine = t // (nt // z.seqs)
    other = z.seqs - 1 - mine
    if not compute:
        x_event(1)
        w_wait(0, 0); w_start(0, 1); w_start(2, 0)
        w_wait(1, 0); w_wait(0, 1); w_start(1, 1); w_start(0, 2)
        x_event(2)
        w_wait(2, 0); w_wait(1, 1); w_start(2, 1); w_start(1, 2)
        x_event(3)
        w_wait(0, 2); w_wait(1, 2); w_wait(2, 1); w_start(2, 2)
        c_event(1)
        w_wait(2, 2)
        c_event(2)
        c_event(3)
    else:
        small[...] = jnp.zeros_like(small)
        vectors()
        w_wait(0, 0); w_start(0, 1); w_start(2, 0)
        x_event(1)
        layer_norm(mine)
        w_wait(1, 0); w_wait(0, 1); w_start(1, 1); w_start(0, 2)
        w_wait(0, 2)
        qkv_tiles(mine)
        x_event(2)
        attend(mine)
        w_wait(2, 0); w_wait(1, 1); w_start(2, 1); w_start(1, 2)
        x_event(3)
        layer_norm(other)
        put(nm, normed_o); put(xh, xhat_o)
        qkv_tiles(other)
        put(qkv, qkv_o)
        w_wait(1, 2)
        put(w.at[:, pl.ds(0, z.n1)], w1_o)
        up_tiles(mine, 0, z.f // 512)
        c_event(1)
        w_wait(2, 1); w_start(2, 2)
        up_tiles(other, 0, z.f // 512)
        put(act, act_o)
        attend(other)
        put(ctx, ctx_o)
        w_wait(2, 2)
        line_sent(xs, 0)
        branch_tiles(mine)
        c_event(2)
        branch_tiles(other)
        put(xs, branch_o)
        grad_tiles(mine)
        c_event(3)
        put(cs, cot_o)
        grad_tiles(other)
        small[2:3, :z.d] = vec[0:1, :]
        small[3:4, :z.d] = vec[2:3, :] + vec[3:4, :]
        put(hg, hg_o); put(dctx, dctx_o); put(small, small_o)

    for cond, copy in waits:
        copy.wait_send()
    line_sent(cs, 1)
    if not compute:
        line_sent(xs, 0)
        put(xs, normed_o); put(xs, xhat_o); put(cs, cot_o); put(w.at[:, pl.ds(0, z.n1)], w1_o)
    for copy in outs:
        copy.wait()


def packed(z, ln_gain, ln_bias, dense_bias, fc2_bias, fc1_bias, qkv_bias):
    lanes, per, base, frows, qrows = pack_rows(z)
    me = lax.axis_index("dp")
    mine = jnp.arange(z.n)[None, :, None] == me
    def spread(a):
        rows, cols = a.reshape(-1, a.shape[-1]).shape
        return jnp.where(mine, a.reshape(rows, 1, cols), BF16(0)).reshape(-1, 128)
    plain = jnp.concatenate([v.reshape(per, lanes) for v in (ln_gain, ln_bias, dense_bias, fc2_bias)], axis=0)
    if lanes < 128:
        plain = jnp.pad(plain, ((0, 0), (0, 128 - lanes)))
    rows = jnp.concatenate([plain, spread(fc1_bias), spread(qkv_bias)], axis=0)
    return jnp.pad(rows, ((0, -rows.shape[0] % 16), (0, 0)))


def forward(z, compute, x, cot, wq, wu, wd, pack):
    prows = pack.shape[0]
    shape = lambda s, dt=BF16: jax.ShapeDtypeStruct(s, dt)
    T = z.rows
    outs = [shape((T, z.d)), shape((T, z.d)), shape((T, z.d)), shape((T, z.q3)), shape((T, z.f)), shape((T, z.f)),
            shape((T, z.c)), shape((T, z.c)), shape((T, z.d)), shape((z.d, z.n1)), shape((8, max(z.d, z.f)), F32)]
    v = pltpu.VMEM
    sem = pltpu.SemaphoreType.DMA
    scratch = [v((z.d, z.n1 + z.n2), BF16), v((T, z.d), BF16), v((T, z.d), BF16), v((T, z.d), BF16), v((T, z.q3), BF16),
               v((T, z.f), BF16), v((T, z.f), BF16), v((T, z.c), BF16), v((T, z.c), BF16), v((T, z.d), BF16),
               v((z.n, prows, 128), BF16), v((8, z.d), F32), v((1, z.n1), F32), v((8, max(z.d, z.f)), F32),
               sem((6,)), sem((12,)), sem((z.n,)), sem((z.n,)), sem((6 * z.n,)), sem((6 * z.n,)), sem((4 * z.nt,)), sem((4 * z.nt,))]
    return pl.pallas_call(
        functools.partial(forward_kernel, z, compute),
        out_shape=outs,
        in_specs=[ANY] * 6 + [VMEM] * 3,
        out_specs=[ANY] * len(outs),
        scratch_shapes=scratch,
        compiler_params=pltpu.CompilerParams(collective_id=0, has_side_effects=True, vmem_limit_bytes=67_043_328),
        name="forward_kernel",
    )(x, cot, wq, wu, wd, pack, *(jnp.asarray(p) for p in rotary_rows()))


def xor(a, b, bits):
    result = 0
    for j in range(bits):
        result = result + (((a // (1 << j)) + (b // (1 << j))) % 2) * (1 << j)
    return result


def grad_chunks(z):
    def cut(width, most=1536):
        pieces, at = [], 0
        while at < width:
            size = min(most, width - at)
            pieces.append((at, size))
            at += size
        return pieces
    chunks = [(False, at, z.n1 + at, size) for at, size in cut(z.n2)]
    chunks += [(True, z.q3 + at, z.q3 + at, size) for at, size in cut(z.f, 1024)]
    chunks += [(True, at, at, size) for at, size in cut(z.q3)]
    return chunks


def kept(order, stage):
    free = [b for b in order[stage:]]
    return sorted(span(free))


def halving_slots(z, h):
    slots = {}
    for stage in range(1, z.bits - 1):
        for m in kept(z.orders_back[h], stage + 1):
            slots[(stage, m)] = len(slots)
    return slots


def backward_kernel(z, *refs):
    (x_hbm, c_hbm, normed_h, xhat_h, cot_h, qkv_h, act_h, hg_h, ctx_h, dctx_h, branch_h, w1_h, small_h, t_here, t_above, t_below,
     out_o, ig_o, own_o, rec_o, sums_o, land1_o, land2_o, landz_o,
     big, left, nm, qkv, dctx, part, send1, stage1, stage2, ng, sta, stb, xh, fin, small, peers, row,
     ld, ld2, out_sem, s1s, s1r, s2s, s2r, zs, zr, vs, vr, ts, tr) = refs
    n, nt, R, D = z.n, z.nt, z.unit, z.d
    me, t = lax.axis_index("dp"), lax.axis_index("tensor")
    T, half_n, shard = z.rows, n // 2, z.shard
    chunks = grad_chunks(z)

    barrier = pltpu.get_barrier_semaphore()
    for m in range(1, n):
        pl.semaphore_signal(barrier, inc=1, device_id={"dp": flip(me, m)}, device_id_type=pl.DeviceIdType.MESH)
    for step in range(1, nt):
        pl.semaphore_signal(barrier, inc=1, device_id={"tensor": lax.rem(t + step, nt)}, device_id_type=pl.DeviceIdType.MESH)

    def load(src, dst, k):
        copy = pltpu.make_async_copy(src, dst, ld.at[k])
        copy.start()
        return copy

    cot_at = big.at[pl.ds(0, T), pl.ds(0, D)]
    act_at = big.at[pl.ds(T, T), pl.ds(0, z.f)]
    ctx_at = big.at[pl.ds(T, T), pl.ds(z.f, z.c)]
    first = [load(cot_h, cot_at, 0), load(act_h, act_at, 1), load(ctx_h, ctx_at, 2)]
    second = [load(normed_h, nm, 3), load(hg_h, left.at[:, pl.ds(z.q3, z.f)], 4), load(small_h, small, 5)]
    third = [load(qkv_h, qkv, 6), load(dctx_h, dctx, 7)]
    pl.semaphore_wait(barrier, n - 1 + nt - 1)

    def remote(src, dst, send, recv, where):
        return pltpu.make_async_remote_copy(
            src_ref=src, dst_ref=dst, send_sem=send, recv_sem=recv, device_id=where, device_id_type=pl.DeviceIdType.MESH
        )

    def unit_rows(u):
        return pl.ds(pl.multiple_of(u * R, R), R)

    def place(up):
        return t if up else nt - 1 - t

    def real_unit(u, up):
        return u if up else nt - 1 - u

    def z_copy(phase, up, k, src):
        i = (phase * 2 + (0 if up else 1)) * nt + k
        slot = landz_o.at[phase, 0 if up else 1, k - 1]
        return remote(slot if src is None else src, slot, zs.at[i], zr.at[i], {"tensor": (t + 1) if up else (t - 1)})

    def z_own(phase, u):
        return (branch_h if phase == 0 else ng).at[unit_rows(u), :]

    def z_edge(phase, k, up):
        @pl.when(place(up) == 0)
        def _():
            z_copy(phase, up, k, z_own(phase, real_unit(nt - k, up))).start()

    def add_rows(dst, src, rows, block=32):
        def body(i, _):
            at = pl.ds(pl.multiple_of(i * block, block), block)
            dst[at, :] = (dst[at, :].astype(F32) + src[at, :].astype(F32)).astype(BF16)
            return 0
        lax.fori_loop(0, rows // block, body, 0)

    def z_forward(phase, k):
        for up in (True, False):
            e = place(up)
            a = sta.at[0 if up else 1]

            @pl.when((e >= 1) & (e <= k))
            def _():
                if k > 1:
                    @pl.when(e <= k - 1)
                    def _():
                        z_copy(phase, up, k, a).wait_send()
                z_copy(phase, up, k, None).wait_recv()
                got = pltpu.make_async_copy(landz_o.at[phase, 0 if up else 1, k - 1], a, ld2.at[0])
                got.start()
                u = real_unit(nt - 1 + e - k, up)
                if phase == 0:
                    mine = pltpu.make_async_copy(z_own(0, u), stb, ld2.at[1])
                    mine.start()
                    mine.wait()
                got.wait()
                add_rows(a, stb if phase == 0 else ng.at[unit_rows(u), :], R)
                z_copy(phase, up, k + 1, a).start()

    def z_last(phase):
        k = nt - 1
        for up in (True, False):
            e = place(up)
            a = sta.at[0 if up else 1]

            @pl.when(e >= 1)
            def _():
                if k > 1:
                    @pl.when(e <= k - 1)
                    def _():
                        z_copy(phase, up, k, a).wait_send()
                z_copy(phase, up, k, None).wait_recv()
                got = pltpu.make_async_copy(landz_o.at[phase, 0 if up else 1, k - 1], a, ld2.at[0])
                got.start()
                got.wait()

            @pl.when(e < 1)
            def _():
                a[...] = jnp.zeros_like(a)

    def z_edges_sent(phase):
        for up in (True, False):
            for k in range(1, nt):
                @pl.when(place(up) == 0)
                def _():
                    z_copy(phase, up, k, z_own(phase, real_unit(nt - k, up))).wait_send()

    for k in range(1, nt):
        for up in (True, False):
            z_edge(0, k, up)

    slot_of = [halving_slots(z, h) for h in (0, 1)]
    n_slots = len(slot_of[0])

    def s1_copy(c, j):
        col, width = chunks[c][2:]
        i = c * half_n + j
        return remote(send1.at[j, :, pl.ds(0, width)], land1_o.at[j, :, pl.ds(col, width)], s1s.at[i], s1r.at[i], {"dp": flip(me, 1)})

    def s2_copy(c, h, stage, m, receive):
        col, width = chunks[c][2:]
        half = width // 2
        cols = pl.ds(col + h * half, half)
        bit = z.orders_back[h][stage]
        kept_m = m if receive else m & ~(1 << bit)
        final = stage == z.bits - 1
        slot = n_slots if final else slot_of[h][(stage, kept_m)]
        dst = rec_o.at[:, cols] if final else land2_o.at[slot, :, cols]
        src = dst if receive else part.at[m >> 1, :, cols]
        i = (c * 2 + h) * (n_slots + 1) + slot
        return remote(src, dst, s2s.at[i], s2r.at[i], {"dp": flip(me, 1 << bit)})

    block = max(shard, 128)

    def tile_of(c, d, h):
        normed, at, col, width = chunks[c]
        half = width // 2
        begin = d * shard
        if shard < 128:
            begin = (begin // 128) * 128
        cols = pl.ds(pl.multiple_of(begin, 128), block)
        if normed:
            tile = dot(nm[:, cols], left[:, pl.ds(at + h * half, half)], TN)
        else:
            tile = dot(big[pl.ds(0, T), cols], big[pl.ds(T, T), pl.ds(at + h * half, half)], TN)
        if shard < 128:
            row[:, pl.ds(0, half)] = tile
            tile = row[pl.ds(pl.multiple_of(d * shard - begin, shard), shard), pl.ds(0, half)]
        return tile

    def dw_send(c):
        width = chunks[c][3]
        half = width // 2

        def body(j, _):
            if c > 0:
                s1_copy(c - 1, j).wait_send()
            d = xor(me, 2 * j + 1, z.bits)
            for h in (0, 1):
                send1[j, :, pl.ds(h * half, half)] = tile_of(c, d, h).astype(BF16)
            s1_copy(c, j).start()
            return 0

        lax.fori_loop(0, half_n, body, 0)

    def dw_own(c):
        col, width = chunks[c][2:]
        half = width // 2

        def body(i, _):
            j = half_n - 1 - i
            d = xor(me, 2 * j, z.bits)
            s1_copy(c, j).wait_recv()
            fetch = pltpu.make_async_copy(land1_o.at[j, :, pl.ds(col, width)], stage1.at[:, pl.ds(0, width)], ld2.at[2])
            fetch.start()
            tiles = [tile_of(c, d, 0)]
            fetch.wait()
            tiles.append(tile_of(c, d, 1))
            for h in (0, 1):
                cols = pl.ds(col + h * half, half)
                part[j, :, cols] = (tiles[h] + stage1[:, pl.ds(h * half, half)].astype(F32)).astype(BF16)
                bit = z.orders_back[h][1]
                for m in kept(z.orders_back[h], 1):
                    if m & (1 << bit):
                        @pl.when(2 * j == m)
                        def _():
                            s2_copy(c, h, 1, m, False).start()
            return 0

        lax.fori_loop(0, half_n, body, 0)

    def dw_combine(c):
        col, width = chunks[c][2:]
        half = width // 2
        for stage in range(1, z.bits - 1):
            jobs = []
            for h in (0, 1):
                for m in kept(z.orders_back[h], stage + 1):
                    k = len(jobs)
                    s2_copy(c, h, stage, m, True).wait_recv()
                    cols = pl.ds(col + h * half, half)
                    fetch = pltpu.make_async_copy(land2_o.at[slot_of[h][(stage, m)], :, cols], stage2.at[k, :, pl.ds(0, half)], ld2.at[3 + k])
                    fetch.start()
                    jobs.append((h, m, cols, fetch))
            jobs_order = sorted(range(len(jobs)), key=lambda k: jobs[k][1] == 0)
            for k in jobs_order:
                h, m, cols, fetch = jobs[k]
                fetch.wait()
                add_rows(part.at[m >> 1, :, cols], stage2.at[k, :, pl.ds(0, half)], shard)
                if m & (1 << z.orders_back[h][stage + 1]):
                    s2_copy(c, h, stage + 1, m, False).start()
        put(part.at[0, :, pl.ds(col, width)], own_o.at[:, pl.ds(col, width)])

    outs = []

    def put(src, dst):
        copy = pltpu.make_async_copy(src, dst, out_sem.at[len(outs)])
        copy.start()
        outs.append(copy)

    half_rows = LEN // 2

    def attend_back(seq):
        low = lax.broadcasted_iota(jnp.int32, (half_rows, 128), 1) < HD
        low_all = lax.broadcasted_iota(jnp.int32, (LEN, 128), 1) < HD

        def pair(p, _):
            def block_of(part_at, start, count):
                cols = pl.ds(pl.multiple_of(part_at * z.c + p * 128, 128), 128)
                return qkv[pl.ds(pl.multiple_of(seq * LEN + start, half_rows), count), cols]

            pcols = pl.ds(pl.multiple_of(p * 128, 128), 128)
            dqs, dks, dvs = [], [None, None], [None, None]
            for qb in range(2):
                keys = half_rows * (qb + 1)
                q2 = block_of(0, qb * half_rows, half_rows)
                k2 = block_of(1, 0, keys)
                v2 = block_of(2, 0, keys)
                g2 = dctx[pl.ds(pl.multiple_of(seq * LEN + qb * half_rows, half_rows), half_rows), pcols]
                rowi = lax.broadcasted_iota(jnp.int32, (half_rows, keys), 0) + qb * half_rows
                seen = lax.broadcasted_iota(jnp.int32, (half_rows, keys), 1) <= rowi
                dq = []
                for side in range(2):
                    keep = low if side == 0 else ~low
                    scores = jnp.where(seen, dot(jnp.where(keep, q2 * BF16(0.125), BF16(0)), k2, NT), -1e30)
                    peak = jnp.max(scores, axis=1, keepdims=True)
                    e = jnp.exp(scores - peak)
                    prob = e * (1.0 / jnp.sum(e, axis=1, keepdims=True))
                    grad = dot(jnp.where(keep, g2, BF16(0)), v2, NT)
                    delta = jnp.sum(prob * grad, axis=1, keepdims=True)
                    ds = (prob * (grad - delta) * 0.125).astype(BF16)
                    dq.append(dot(ds, k2, NN))
                    dk = dot(ds, q2, TN)
                    dv = dot(prob.astype(BF16), g2, TN)
                    if qb == 0:
                        dks[side], dvs[side] = dk, dv
                    else:
                        zero = jnp.zeros((half_rows, 128), F32)
                        dks[side] = dk + jnp.concatenate([dks[side], zero], axis=0)
                        dvs[side] = dv + jnp.concatenate([dvs[side], zero], axis=0)
                dqs.append(jnp.where(low, dq[0], dq[1]))
            rows = pl.ds(pl.multiple_of(seq * LEN, LEN), LEN)
            grads = (jnp.concatenate(dqs, axis=0), jnp.where(low_all, dks[0], dks[1]), jnp.where(low_all, dvs[0], dvs[1]))
            for which, value in enumerate(grads):
                if which < 2:
                    value = rotated(value, t_here[...], -t_above[...], -t_below[...])
                cols = pl.ds(pl.multiple_of(which * z.c + p * 128, 128), 128)
                small[4:5, cols] += jnp.sum(value, axis=0, keepdims=True)
                left[rows, cols] = value.astype(BF16)
            return 0

        lax.fori_loop(0, z.c // 128, pair, 0)

    def ng_tiles(seq):
        rows = pl.ds(pl.multiple_of(seq * LEN, LEN), LEN)
        fetch = pltpu.make_async_copy(xhat_h.at[rows, :], xh, ld2.at[0])
        fetch.start()
        fetch.wait()

        def body(j, _):
            cols = pl.ds(pl.multiple_of(j * 512, 512), 512)
            tile = dot(left[rows, :], big[cols, :], NT)
            small[5:6, cols] += jnp.sum(tile * xh[:, cols].astype(F32), axis=0, keepdims=True)
            small[6:7, cols] += jnp.sum(tile, axis=0, keepdims=True)
            ng[rows, cols] = tile.astype(BF16)
            return 0

        lax.fori_loop(0, D // 512, body, 0)

    def v_copy(m, receive):
        slot = peers.at[flip(me, m)] if receive else peers.at[me]
        return remote(small, slot, vs.at[m], vr.at[m], {"dp": flip(me, m)})

    def t_copy(k, receive):
        to = lax.rem(t + k, nt)
        slot = peers.at[n + (lax.rem(t + nt - k, nt) if receive else t)]
        return remote(fin.at[pl.ds(0, 8), :], slot, ts.at[k], tr.at[k], {"tensor": to})

    def sums_over_group():
        for m in range(1, n):
            v_copy(m, True).wait_recv()
        total = small[...]
        for m in range(1, n):
            total = total + peers[flip(me, m)]
        fin[pl.ds(0, 8), :] = total
        for k in range(1, nt):
            t_copy(k, False).start()

    def sums_over_all():
        total = fin[pl.ds(0, 8), :]
        rest = jnp.zeros_like(total)
        for k in range(1, nt):
            t_copy(k, True).wait_recv()
            rest = rest + peers[n + lax.rem(t + nt - k, nt)]
        line = lax.broadcasted_iota(jnp.int32, total.shape, 0)
        small[...] = jnp.where(line == 2, small[...], jnp.where(line >= 5, total + rest, total))
        for k in range(1, nt):
            t_copy(k, False).wait_send()

    def finish_out():
        got = pltpu.make_async_copy(z_own(0, t), stb, ld2.at[0])
        got.start()
        mine = pltpu.make_async_copy(x_hbm, xh.at[pl.ds(0, R), :], ld2.at[1])
        mine.start()
        got.wait()
        mine.wait()

        def body(i, _):
            at = pl.ds(pl.multiple_of(i * 16, 16), 16)
            total = xh[at, :].astype(F32) + (stb[at, :].astype(F32) + sta[0, at, :].astype(F32) + sta[1, at, :].astype(F32))
            stb[at, :] = (total + small[3:4, :D]).astype(BF16)
            return 0

        lax.fori_loop(0, R // 16, body, 0)
        copy = pltpu.make_async_copy(stb, out_o, ld2.at[0])
        copy.start()
        copy.wait()

    def finish_grad():
        def body(i, _):
            at = pl.ds(pl.multiple_of(i * 16, 16), 16)
            full = xh[at, :].astype(F32)
            centred = full - jnp.mean(full, axis=1, keepdims=True)
            inv_std = lax.rsqrt(jnp.mean(centred * centred, axis=1, keepdims=True) + EPSILON)
            hat = centred * inv_std
            grad = ng[pl.ds(pl.multiple_of(t * R + i * 16, 16), 16), :].astype(F32)
            grad = (grad + sta[0, at, :].astype(F32) + sta[1, at, :].astype(F32)) * small[2:3, :D]
            middle = jnp.mean(grad, axis=1, keepdims=True)
            along = jnp.mean(grad * hat, axis=1, keepdims=True)
            fin[at, :] = stb[at, :].astype(F32) + inv_std * (grad - middle - hat * along)
            return 0

        lax.fori_loop(0, R // 16, body, 0)
        copy = pltpu.make_async_copy(fin, ig_o, ld2.at[0])
        copy.start()
        copy.wait()

    mine = t // (nt // z.seqs)
    other = z.seqs - 1 - mine
    two = sum(1 for chunk in chunks if not chunk[0])
    up_chunks = [c for c, chunk in enumerate(chunks) if chunk[0] and chunk[1] >= z.q3]
    qkv_chunks = [c for c, chunk in enumerate(chunks) if chunk[0] and chunk[1] < z.q3]

    for copy in first:
        copy.wait()
    for c in range(two):
        dw_send(c)
        dw_own(c)
    wload = load(w1_h, big, 8)
    for copy in second + third:
        copy.wait()
    small[4:8, :] = jnp.zeros((4, small.shape[1]), F32)
    z_forward(0, 1)
    dw_combine(0)
    for c in up_chunks:
        dw_send(c)
        dw_own(c)
    attend_back(other)
    z_forward(0, 2)
    dw_combine(1)
    attend_back(mine)
    dw_combine(2)
    wload.wait()
    ng_tiles(other)
    z_last(0)
    finish_out()
    for k in range(1, nt - 1):
        for up in (True, False):
            z_edge(1, k, up)
    ng_tiles(mine)
    for up in (True, False):
        z_edge(1, nt - 1, up)
    for c in qkv_chunks:
        dw_send(c)
        for m in range(1, n):
            if c == qkv_chunks[0]:
                v_copy(m, False).start()
        dw_own(c)
    z_forward(1, 1)
    dw_combine(3)
    sums_over_group()
    z_forward(1, 2)
    for c in range(4, len(chunks)):
        dw_combine(c)
    for m in range(1, n):
        v_copy(m, False).wait_send()
    sums_over_all()
    put(small, sums_o)
    last_x = load(x_hbm, xh.at[pl.ds(0, R), :], 9)
    last_c = load(c_hbm, stb, 10)
    last_x.wait()
    last_c.wait()
    for c in range(len(chunks)):
        for h in (0, 1):
            s2_copy(c, h, z.bits - 1, 0, True).wait_recv()
    z_last(1)
    for c in range(len(chunks)):
        for h in (0, 1):
            for stage in range(1, z.bits):
                for m in kept(z.orders_back[h], stage):
                    if m & (1 << z.orders_back[h][stage]):
                        s2_copy(c, h, stage, m, False).wait_send()
    for j in range(half_n):
        s1_copy(len(chunks) - 1, j).wait_send()
    z_edges_sent(0)
    z_edges_sent(1)
    finish_grad()
    for copy in outs:
        copy.wait()


def backward(z, x, cot, arrays):
    shape = lambda s, dt=BF16: jax.ShapeDtypeStruct(s, dt)
    T, W = z.rows, z.n1 + z.n2
    width = max(z.d, z.f)
    half_n = z.n // 2
    chunks = grad_chunks(z)
    most = max(chunk[3] for chunk in chunks)
    n_slots = len(halving_slots(z, 0))
    outs = [shape((z.unit, z.d)), shape((z.unit, z.d), F32), shape((z.shard, W)), shape((z.shard, W)), shape((8, width), F32),
            shape((half_n, z.shard, W)), shape((n_slots, z.shard, W)), shape((2, 2, z.nt - 1, z.unit, z.d))]
    v = pltpu.VMEM
    sem = pltpu.SemaphoreType.DMA
    nc = len(chunks)
    scratch = [v((z.d, z.n1), BF16), v((T, z.n1), BF16), v((T, z.d), BF16), v((T, z.q3), BF16), v((T, z.c), BF16),
               v((half_n, z.shard, W), BF16), v((half_n, z.shard, most), BF16), v((z.shard, most), BF16),
               v((z.n // 2, z.shard, most // 2), BF16), v((T, z.d), BF16), v((2, z.unit, z.d), BF16), v((z.unit, z.d), BF16),
               v((LEN, z.d), BF16), v((z.unit, z.d), F32), v((8, width), F32), v((z.n + z.nt, 8, width), F32), v((128, most // 2), F32),
               sem((11,)), sem((3 + z.n // 2,)), sem((nc + 2,)), sem((nc * half_n,)), sem((nc * half_n,)),
               sem((nc * 2 * (n_slots + 1),)), sem((nc * 2 * (n_slots + 1),)), sem((4 * z.nt,)), sem((4 * z.nt,)),
               sem((z.n,)), sem((z.n,)), sem((z.nt,)), sem((z.nt,))]
    return pl.pallas_call(
        functools.partial(backward_kernel, z),
        out_shape=outs,
        in_specs=[ANY] * 13 + [VMEM] * 3,
        out_specs=[ANY] * len(outs),
        scratch_shapes=scratch,
        compiler_params=pltpu.CompilerParams(collective_id=1, has_side_effects=True, vmem_limit_bytes=67_043_328),
        name="backward_kernel",
    )(x, cot, *arrays, *(jnp.asarray(p) for p in rotary_rows()))


def shards(x, ln_gain, ln_bias, qkv_weight, qkv_bias, dense_weight, dense_bias, fc1_weight, fc1_bias, fc2_weight, fc2_bias, cotangent):
    z = Sizes(lax.axis_size("dp"), lax.axis_size("tensor"), x.shape[0], x.shape[1], fc1_weight.shape[1], dense_weight.shape[0])
    pack = packed(z, ln_gain, ln_bias, dense_bias, fc2_bias, fc1_bias, qkv_bias)
    wd = jnp.concatenate([fc2_weight.T, dense_weight.T], axis=1)
    arrays = forward(z, True, x, cotangent, qkv_weight.reshape(z.shard, z.q3), fc1_weight, wd, pack)
    hidden_out, input_grad, own, rec, sums = backward(z, x, cotangent, arrays)[:5]
    dw = own.astype(F32) + rec.astype(F32)
    i, t = lax.axis_index("dp"), lax.axis_index("tensor")
    piece = z.d // (z.n * z.nt)
    cut = lambda r: lax.dynamic_slice(sums, (r, (i * z.nt + t) * piece), (1, piece)).reshape(piece)
    hc = HD // z.n
    fb = lax.dynamic_slice_in_dim(sums[1, :z.f].reshape(-1, HD), i * hc, hc, 1)
    qb = lax.dynamic_slice_in_dim(sums[4, :z.q3].reshape(3, -1, HD), i * hc, hc, 2)
    dbias = cut(0)
    return (hidden_out, input_grad, dw[:, :z.q3].reshape(z.shard, 3, z.c), qb, dw[:, z.n1 + z.f:].T, dbias, dw[:, z.q3:z.n1], fb,
            dw[:, z.n1:z.n1 + z.f].T, dbias, cut(5), cut(6))


def solution(mesh):
    both = ("dp", "tensor")
    placed = (
        P(both, None), P("dp"), P("dp"), P("dp", None, "tensor"), P(None, "tensor", "dp"), P("tensor", "dp"),
        P("dp"), P("dp", "tensor"), P("tensor", "dp"), P("tensor", "dp"), P("dp"), P(both, None),
    )
    given = (
        P(both, None), P(both, None), P("dp", None, "tensor"), P(None, "tensor", "dp"), P("tensor", "dp"), P(both),
        P("dp", "tensor"), P("tensor", "dp"), P("tensor", "dp"), P(both), P(both), P(both),
    )
    return jax.shard_map(shards, mesh=mesh, in_specs=placed, out_specs=given, check_vma=False)
```

```python
import functools
import math

import jax
import jax.numpy as jnp
import numpy as np
from jax import lax
from jax.experimental import pallas as pl
from jax.experimental.pallas import tpu as pltpu
from jax.sharding import PartitionSpec as P

HD = 64
ROT = 32
LEN = 512
EPSILON = 1e-05
GELU_C = math.sqrt(2.0 / math.pi)
F32 = jnp.float32
BF16 = jnp.bfloat16
ANY = pl.BlockSpec(memory_space=pl.ANY)
VMEM = pl.BlockSpec(memory_space=pltpu.VMEM)


def gelu_pair(h):
    square = h * h
    tangent = jnp.tanh(h * (GELU_C + (GELU_C * 0.044715) * square))
    half = 0.5 + 0.5 * tangent
    slope = half + 0.5 * h * (1.0 - tangent * tangent) * (GELU_C + (3.0 * 0.044715 * GELU_C) * square)
    return h * half, slope


def rotary_rows():
    position = np.arange(LEN, dtype=np.float32)
    frequency = (10000.0 ** (-np.arange(0, ROT, 2, dtype=np.float32) / ROT)).astype(np.float32)
    angles = (position[:, None] * frequency[None, :]).astype(np.float32)
    cosine, sine = np.cos(angles).astype(np.float32), np.sin(angles).astype(np.float32)
    rest = np.ones((LEN, HD - ROT), np.float32)
    none = np.zeros((LEN, ROT // 2), np.float32)
    here = np.concatenate([cosine, cosine, rest], axis=1)
    above = np.concatenate([-sine, none, 0 * rest], axis=1)
    below = np.concatenate([none, sine, 0 * rest], axis=1)
    return tuple(np.tile(part, (1, 2)) for part in (here, above, below))


def flip(index, mask):
    result, place = index, 1
    while place <= mask:
        if mask & place:
            result = result + (1 - 2 * ((index // place) % 2)) * place
        place *= 2
    return result


def span(bits):
    masks = [0]
    for bit in bits:
        masks = masks + [mask | (1 << bit) for mask in masks]
    return masks


def dot(a, b, dims):
    return lax.dot_general(a, b, (dims, ((), ())), preferred_element_type=F32)


NN, NT, TN = ((1,), (0,)), ((1,), (1,)), ((0,), (0,))


class Sizes:
    def __init__(self, groups, tensor, unit, width, hidden, heads_width):
        self.n, self.nt = groups, tensor
        self.bits = groups.bit_length() - 1
        self.unit, self.d, self.f, self.c = unit, width, hidden, heads_width
        self.rows = unit * tensor
        self.seqs = self.rows // LEN
        self.shard = width // groups
        self.q3 = 3 * heads_width
        self.n1 = self.q3 + hidden
        self.n2 = hidden + heads_width
        self.orders = (
            list(range(1, self.bits)) + [0],
            list(range(self.bits - 1, 0, -1)) + [0],
        )
        self.orders_back = tuple(list(reversed(order)) for order in self.orders)


def pack_rows(z):
    lanes = min(128, z.shard)
    per = z.shard // lanes
    return lanes, per, 4 * per, z.f // 128, z.q3 // 128


def rotated(tile, here, above, below):
    width = tile.shape[1]
    up = pltpu.roll(tile, width - ROT // 2, axis=1)
    down = pltpu.roll(tile, ROT // 2, axis=1)
    repeat = width // 128
    return (
        tile * jnp.tile(here, (1, repeat))
        + up * jnp.tile(above, (1, repeat))
        + down * jnp.tile(below, (1, repeat))
    )


def xor(a, b, bits):
    result = 0
    for j in range(bits):
        result = result + (((a // (1 << j)) + (b // (1 << j))) % 2) * (1 << j)
    return result


def kept(order, stage):
    free = [b for b in order[stage:]]
    return sorted(span(free))


def halving_slots(z, h):
    slots = {}
    for stage in range(1, z.bits - 1):
        for m in kept(z.orders_back[h], stage + 1):
            slots[(stage, m)] = len(slots)
    return slots


def grad_chunks(z):
    def cut(kind, at, col, width):
        pieces, start = [], 0
        while start < width:
            size = min(1024, width - start)
            pieces.append((kind, at + start, col + start, size))
            start += size
        return pieces
    return cut("act", 0, z.n1, z.f) + cut("ctx", 0, z.n1 + z.f, z.c) + cut("left", z.q3, z.q3, z.f) + cut("left", 0, 0, z.q3)


def block_kernel(z, *refs):
    (x_hbm, c_hbm, wq_hbm, wu_hbm, wd_hbm, wo_hbm, pack_hbm, t_here, t_above, t_below,
     out_o, ig_o, own_o, rec_o, sums_o, land1_o, land2_o, landz_o, xhat_o,
     w, xs, cs, qkv, act, left, ctx, nm, slots, vec, bias, small, send1, stage1, stage2, sta, stb, fin, tot, peers, row,
     loc, ld2, out_sem, pk_send, pk_recv, w_send, w_recv, z_send, z_recv, s1s, s1r, s2s, s2r, zs, zr, vs, vr, ts, tr) = refs
    ng = act
    n, nt, R, D, T = z.n, z.nt, z.unit, z.d, z.rows
    half_n, shard, last = n // 2, z.shard, z.bits - 1
    me, t = lax.axis_index("dp"), lax.axis_index("tensor")
    chunks = grad_chunks(z)

    def remote(src, dst, send, recv, where):
        return pltpu.make_async_remote_copy(
            src_ref=src, dst_ref=dst, send_sem=send, recv_sem=recv, device_id=where, device_id_type=pl.DeviceIdType.MESH
        )

    def rows_of(u):
        return pl.ds(pl.multiple_of(u * R, R), R)

    def seq_rows(seq):
        return pl.ds(pl.multiple_of(seq * LEN, LEN), LEN)

    barrier = pltpu.get_barrier_semaphore()
    for m in range(1, n):
        pl.semaphore_signal(barrier, inc=1, device_id={"dp": flip(me, m)}, device_id_type=pl.DeviceIdType.MESH)
    for step in range(1, nt):
        pl.semaphore_signal(barrier, inc=1, device_id={"tensor": lax.rem(t + step, nt)}, device_id_type=pl.DeviceIdType.MESH)

    wchunks = [(wq_hbm, 0, z.q3), (wo_hbm, z.n1 + z.f, z.c), (wu_hbm, z.q3, z.f), (wd_hbm, z.n1, z.f)]
    Q, O, U, Dn = range(4)

    def slot_ref(d, col, width):
        return w.at[pl.ds(pl.multiple_of(d * shard, shard), shard), pl.ds(col, width)]

    own_copies = [
        pltpu.make_async_copy(x_hbm, xs.at[rows_of(t), :], loc.at[0]),
        pltpu.make_async_copy(c_hbm, cs.at[rows_of(t), :], loc.at[1]),
        pltpu.make_async_copy(pack_hbm, slots.at[me], loc.at[2]),
    ] + [pltpu.make_async_copy(src, slot_ref(me, col, width), loc.at[3 + c]) for c, (src, col, width) in enumerate(wchunks)]
    for copy in own_copies:
        copy.start()
    pl.semaphore_wait(barrier, n - 1 + nt - 1)

    def w_copy(c, h, bit, m, receive):
        src_hbm, col, width = wchunks[c]
        half = width // 2
        col = col + h * half
        d = flip(me, m | (1 << bit)) if receive else flip(me, m)
        dst = slot_ref(d, col, half)
        src = src_hbm.at[:, pl.ds(h * half, half)] if m == 0 and not receive else dst
        s = (c * 2 + h) * n + (m | (1 << bit))
        return remote(src, dst, w_send.at[s], w_recv.at[s], {"dp": flip(me, 1 << bit)})

    w_sent = [[] for _ in wchunks]

    def w_start(c, stage):
        for h in (0, 1):
            order = z.orders[h]
            sends = [(order[stage], m) for m in span(order[:stage])] if stage < last else []
            fresh = [0] if stage == 0 else [m for m in span(order[:stage]) if m & (1 << order[stage - 1])]
            for bit, m in sends + [(0, m) for m in fresh]:
                copy = w_copy(c, h, bit, m, False)
                copy.start()
                w_sent[c].append(copy)

    def w_step(c, stage):
        for h in (0, 1):
            for m in span(z.orders[h][:stage]):
                w_copy(c, h, z.orders[h][stage], m, True).wait_recv()
        w_start(c, stage + 1)

    def w_rest(c):
        for stage in range(1, last):
            w_step(c, stage)

    def w_ready(c):
        for h in (0, 1):
            for m in span(z.orders[h][:last]):
                w_copy(c, h, 0, m, True).wait_recv()

    def pack_copy(m, receive):
        slot = slots.at[flip(me, m)] if receive else slots.at[me]
        return remote(pack_hbm, slot, pk_send.at[m], pk_recv.at[m], {"dp": flip(me, m)})

    def line(buf, which, j, up, receive):
        src = (t - (j - 1)) if up else (t + (j - 1))
        got = (t - j) if up else (t + j)
        ref = buf.at[rows_of(got if receive else src), :]
        s = (which * 2 + (0 if up else 1)) * nt + j
        from_ref = (x_hbm if which == 0 else c_hbm) if j == 1 and not receive else ref
        return remote(from_ref, ref, z_send.at[s], z_recv.at[s], {"tensor": (t + 1) if up else (t - 1)})

    def sends(j, up):
        return ((t < nt - 1) & (t >= j - 1)) if up else ((t > 0) & (t <= nt - j))

    def gets(j, up):
        return (t >= j) if up else (t <= nt - 1 - j)

    def line_send(buf, which, j, up, extra=None):
        cond = sends(j, up) if extra is None else sends(j, up) & extra

        @pl.when(cond)
        def _():
            line(buf, which, j, up, False).start()

    def line_recv(buf, which, j, up):
        @pl.when(gets(j, up))
        def _():
            line(buf, which, j, up, True).wait_recv()

    def line_sent(buf, which):
        for j in range(1, nt):
            for up in (True, False):
                @pl.when(sends(j, up))
                def _():
                    line(buf, which, j, up, False).wait_send()

    def cot_starts(j):
        line_send(cs, 1, 1, True, t == j)
        line_send(cs, 1, 1, False, t == nt - 1 - j)

    def x_event(j):
        for up in (True, False):
            line_recv(xs, 0, j, up)
        if j < nt - 1:
            for up in (True, False):
                line_send(xs, 0, j + 1, up)
        cot_starts(j)

    def c_event(j):
        for up in (True, False):
            line_recv(cs, 1, j, up)
        if j < nt - 1:
            for up in (True, False):
                line_send(cs, 1, j + 1, up)

    for m in range(1, n):
        pack_copy(m, False).start()
    for up in (True, False):
        line_send(xs, 0, 1, up)
    w_start(Q, 0)
    w_start(O, 0)
    cot_starts(0)
    for m in range(1, n):
        pack_copy(m, True).wait_recv()
    for copy in own_copies:
        copy.wait()

    lanes, per, base, frows, qrows = pack_rows(z)

    def vectors():
        small[...] = jnp.zeros_like(small)
        for v in range(4):
            for d in range(n):
                for r in range(per):
                    at = d * shard + r * lanes
                    vec[pl.ds(v, 1), pl.ds(at, lanes)] = slots[d, pl.ds(v * per + r, 1), :lanes].astype(F32)
        total = jnp.zeros((frows + qrows, 128), F32)
        for d in range(n):
            total = total + slots[d, pl.ds(base, frows + qrows), :].astype(F32)
        for r in range(qrows):
            bias[:, pl.ds(r * 128, 128)] = total[frows + r:frows + r + 1, :]
        for r in range(frows):
            bias[:, pl.ds(z.q3 + r * 128, 128)] = total[r:r + 1, :]
        small[2:3, :D] = vec[0:1, :]
        small[3:4, :D] = vec[2:3, :] + vec[3:4, :]

    def xhat_out(u, slot):
        return pltpu.make_async_copy(sta.at[slot], xhat_o.at[rows_of(u), :], ld2.at[slot])

    def layer_norm(u, slot):
        block = 16

        def body(i, _):
            at = pl.ds(pl.multiple_of(i * block, block), block)
            rows = pl.ds(pl.multiple_of(u * R + i * block, block), block)
            full = xs[rows, :].astype(F32)
            centred = full - jnp.mean(full, axis=1, keepdims=True)
            inv_std = lax.rsqrt(jnp.mean(centred * centred, axis=1, keepdims=True) + EPSILON)
            hat = centred * inv_std
            sta[slot, at, :] = hat.astype(BF16)
            nm[rows, :] = (hat * vec[0:1, :] + vec[1:2, :]).astype(BF16)
            return 0

        lax.fori_loop(0, R // block, body, 0)
        xhat_out(u, slot).start()

    def qkv_tiles(seq):
        rows = seq_rows(seq)
        for part in range(3):
            cols = pl.ds(part * z.c, z.c)
            tile = dot(nm[rows, :], w[:, cols], NN) + bias[:, cols]
            if part < 2:
                tile = rotated(tile, t_here[...], t_above[...], t_below[...])
            qkv[rows, cols] = tile.astype(BF16)

    def up_tiles(seq):
        rows = seq_rows(seq)

        def body(j, _):
            cols = pl.ds(pl.multiple_of(j * 512, 512), 512)
            wcols = pl.ds(pl.multiple_of(z.q3 + j * 512, 512), 512)
            value, slope = gelu_pair(dot(nm[rows, :], w[:, wcols], NN) + bias[:, wcols])
            act[rows, cols] = value.astype(BF16)
            left[rows, wcols] = slope.astype(BF16)
            return 0

        lax.fori_loop(0, z.f // 512, body, 0)

    half_rows = LEN // 2

    def head_pair(seq, p):
        def block(part, start, count):
            cols = pl.ds(pl.multiple_of(part * z.c + p * 128, 128), 128)
            return qkv[pl.ds(pl.multiple_of(seq * LEN + start, half_rows), count), cols]
        return block

    def softmax(q2, k2, keep, start):
        keys = k2.shape[0]
        row_at = lax.broadcasted_iota(jnp.int32, (half_rows, keys), 0) + start
        seen = lax.broadcasted_iota(jnp.int32, (half_rows, keys), 1) <= row_at
        scores = jnp.where(seen, dot(jnp.where(keep, q2 * BF16(0.125), BF16(0)), k2, NT), -1e30)
        e = jnp.exp(scores - jnp.max(scores, axis=1, keepdims=True))
        return e * (1.0 / jnp.sum(e, axis=1, keepdims=True))

    def attend(seq):
        low = lax.broadcasted_iota(jnp.int32, (half_rows, 128), 1) < HD

        def pair(p, _):
            block = head_pair(seq, p)
            for qb in range(2):
                start, keys = qb * half_rows, half_rows * (qb + 1)
                q2, k2, v2 = block(0, start, half_rows), block(1, 0, keys), block(2, 0, keys)
                parts = [dot(softmax(q2, k2, keep, start).astype(BF16), v2, NN) for keep in (low, ~low)]
                ctx[pl.ds(pl.multiple_of(seq * LEN + start, half_rows), half_rows),
                    pl.ds(pl.multiple_of(p * 128, 128), 128)] = jnp.where(low, parts[0], parts[1]).astype(BF16)
            return 0

        lax.fori_loop(0, z.c // 128, pair, 0)

    def branch_tiles(seq):
        rows = seq_rows(seq)

        def body(j, _):
            wrows = pl.ds(pl.multiple_of(j * 512, 512), 512)
            tile = dot(act[rows, :], w[wrows, pl.ds(z.n1, z.f)], NT)
            tile = tile + dot(ctx[rows, :], w[wrows, pl.ds(z.n1 + z.f, z.c)], NT)
            xs[rows, wrows] = tile.astype(BF16)
            return 0

        lax.fori_loop(0, D // 512, body, 0)

    def context_grads(begin, count):
        rows = pl.ds(pl.multiple_of(begin, count), count)
        left[rows, pl.ds(2 * z.c, z.c)] = dot(cs[rows, :], w[:, pl.ds(z.n1 + z.f, z.c)], NN).astype(BF16)

    def hidden_grads(begin, count):
        rows = pl.ds(pl.multiple_of(begin, count), count)

        def body(j, _):
            cols = pl.ds(pl.multiple_of(j * 512, 512), 512)
            gcols = pl.ds(pl.multiple_of(z.q3 + j * 512, 512), 512)
            wcols = pl.ds(pl.multiple_of(z.n1 + j * 512, 512), 512)
            grad = dot(cs[rows, :], w[:, wcols], NN) * left[rows, gcols].astype(F32)
            small[1:2, cols] += jnp.sum(grad, axis=0, keepdims=True)
            left[rows, gcols] = grad.astype(BF16)
            return 0

        lax.fori_loop(0, z.f // 512, body, 0)

    def cot_sums(begin, count):
        def sums(i, _):
            part = cs[pl.ds(pl.multiple_of(begin + i * 64, 64), 64), :].astype(F32)
            small[0:1, :D] += jnp.sum(part, axis=0, keepdims=True)
            return 0

        lax.fori_loop(0, count // 64, sums, 0)

    def attend_back(seq):
        low = lax.broadcasted_iota(jnp.int32, (half_rows, 128), 1) < HD
        low_all = lax.broadcasted_iota(jnp.int32, (LEN, 128), 1) < HD

        def pair(p, _):
            block = head_pair(seq, p)
            gcols = pl.ds(pl.multiple_of(2 * z.c + p * 128, 128), 128)
            dqs, dks, dvs = [], [None, None], [None, None]
            for qb in range(2):
                start, keys = qb * half_rows, half_rows * (qb + 1)
                q2, k2, v2 = block(0, start, half_rows), block(1, 0, keys), block(2, 0, keys)
                g2 = left[pl.ds(pl.multiple_of(seq * LEN + start, half_rows), half_rows), gcols]
                dq = []
                for side, keep in enumerate((low, ~low)):
                    prob = softmax(q2, k2, keep, start)
                    grad = dot(jnp.where(keep, g2, BF16(0)), v2, NT)
                    delta = jnp.sum(prob * grad, axis=1, keepdims=True)
                    ds = (prob * (grad - delta) * 0.125).astype(BF16)
                    dq.append(dot(ds, k2, NN))
                    dk = dot(ds, q2, TN)
                    dv = dot(prob.astype(BF16), g2, TN)
                    if qb:
                        zero = jnp.zeros((half_rows, 128), F32)
                        dk = dk + jnp.concatenate([dks[side], zero], axis=0)
                        dv = dv + jnp.concatenate([dvs[side], zero], axis=0)
                    dks[side], dvs[side] = dk, dv
                dqs.append(jnp.where(low, dq[0], dq[1]))
            grads = (jnp.concatenate(dqs, axis=0), jnp.where(low_all, dks[0], dks[1]), jnp.where(low_all, dvs[0], dvs[1]))
            for which, value in enumerate(grads):
                if which < 2:
                    value = rotated(value, t_here[...], -t_above[...], -t_below[...])
                cols = pl.ds(pl.multiple_of(which * z.c + p * 128, 128), 128)
                small[4:5, cols] += jnp.sum(value, axis=0, keepdims=True)
                left[seq_rows(seq), cols] = value.astype(BF16)
            return 0

        lax.fori_loop(0, z.c // 128, pair, 0)

    def ng_tiles(seq):
        rows = seq_rows(seq)

        def hat(j):
            slot = lax.rem(j, 2) if not isinstance(j, int) else j % 2
            cols = pl.ds(pl.multiple_of(j * 512, 512), 512)
            place = ctx.at[pl.ds(pl.multiple_of(slot * LEN, LEN), LEN), :]
            return place, pltpu.make_async_copy(xhat_o.at[rows, cols], place, ld2.at[slot])

        hat(0)[1].start()

        def body(j, _):
            cols = pl.ds(pl.multiple_of(j * 512, 512), 512)

            @pl.when(j + 1 < D // 512)
            def _():
                hat(j + 1)[1].start()
            tile = dot(left[rows, :], w[cols, pl.ds(0, z.n1)], NT)
            place, copy = hat(j)
            copy.wait()
            small[5:6, cols] += jnp.sum(tile * place[...].astype(F32), axis=0, keepdims=True)
            small[6:7, cols] += jnp.sum(tile, axis=0, keepdims=True)
            ng[rows, cols] = tile.astype(BF16)
            return 0

        lax.fori_loop(0, D // 512, body, 0)

    def place_of(up):
        return t if up else nt - 1 - t

    def real_unit(u, up):
        return u if up else nt - 1 - u

    def z_copy(phase, up, k, src):
        i = (phase * 2 + (0 if up else 1)) * nt + k
        slot = landz_o.at[phase, 0 if up else 1, k - 1]
        return remote(slot if src is None else src, slot, zs.at[i], zr.at[i], {"tensor": (t + 1) if up else (t - 1)})

    def z_own(phase, u):
        return (xs if phase == 0 else ng).at[rows_of(u), :]

    def z_edges(phase, which):
        for k in which:
            for up in (True, False):
                @pl.when(place_of(up) == 0)
                def _():
                    z_copy(phase, up, k, z_own(phase, real_unit(nt - k, up))).start()

    def add_rows(dst, src, rows, block=32):
        def body(i, _):
            at = pl.ds(pl.multiple_of(i * block, block), block)
            dst[at, :] = (dst[at, :].astype(F32) + src[at, :].astype(F32)).astype(BF16)
            return 0
        lax.fori_loop(0, rows // block, body, 0)

    def z_take(phase, k, up, a):
        e = place_of(up)
        if k > 1:
            @pl.when(e <= k - 1)
            def _():
                z_copy(phase, up, k, a).wait_send()
        z_copy(phase, up, k, None).wait_recv()
        got = pltpu.make_async_copy(landz_o.at[phase, 0 if up else 1, k - 1], a, ld2.at[0])
        got.start()
        got.wait()

    def z_forward(phase, k):
        for up in (True, False):
            e = place_of(up)
            a = sta.at[0 if up else 1]

            @pl.when((e >= 1) & (e <= k))
            def _():
                z_take(phase, k, up, a)
                add_rows(a, z_own(phase, real_unit(nt - 1 + e - k, up)), R)
                z_copy(phase, up, k + 1, a).start()

    def z_last(phase):
        for up in (True, False):
            a = sta.at[0 if up else 1]

            @pl.when(place_of(up) >= 1)
            def _():
                z_take(phase, nt - 1, up, a)

            @pl.when(place_of(up) < 1)
            def _():
                a[...] = jnp.zeros_like(a)

    def z_edges_sent(phase):
        for up in (True, False):
            for k in range(1, nt):
                @pl.when(place_of(up) == 0)
                def _():
                    z_copy(phase, up, k, z_own(phase, real_unit(nt - k, up))).wait_send()

    slot_of = [halving_slots(z, h) for h in (0, 1)]
    n_slots = len(slot_of[0])

    def part_ref(c, j, cols, width):
        kind, at = chunks[c][:2]
        if kind != "left":
            buf, first, shift = w, 0, 0
        elif at >= z.q3:
            buf, first, shift = w, D // 2, z.n1 - z.q3
        else:
            buf, first, shift = xs, 0, 0
        begin = first + j * shard
        if not isinstance(j, int):
            begin = pl.multiple_of(begin, shard)
        return buf.at[pl.ds(begin, shard), pl.ds(cols + shift, width)]

    def s1_copy(c, j):
        col, width = chunks[c][2:]
        i = c * half_n + j
        return remote(send1.at[j, :, pl.ds(0, width)], land1_o.at[j, :, pl.ds(col, width)], s1s.at[i], s1r.at[i], {"dp": flip(me, 1)})

    def s2_copy(c, h, stage, m, receive):
        col, width = chunks[c][2:]
        half = width // 2
        at = col + h * half
        bit = z.orders_back[h][stage]
        kept_m = m if receive else m & ~(1 << bit)
        final = stage == z.bits - 1
        slot = n_slots if final else slot_of[h][(stage, kept_m)]
        dst = rec_o.at[:, pl.ds(at, half)] if final else land2_o.at[slot, :, pl.ds(at, half)]
        src = dst if receive else part_ref(c, m >> 1, at, half)
        i = (c * 2 + h) * (n_slots + 1) + slot
        return remote(src, dst, s2s.at[i], s2r.at[i], {"dp": flip(me, 1 << bit)})

    block = max(shard, 128)

    def tile_of(c, d, h):
        kind, at, col, width = chunks[c]
        half = width // 2
        begin = d * shard
        if shard < 128:
            begin = (begin // 128) * 128
        cols = pl.ds(pl.multiple_of(begin, 128), block)
        buf = {"act": act, "ctx": ctx, "left": left}[kind]
        tile = dot((nm if kind == "left" else cs)[:, cols], buf[:, pl.ds(at + h * half, half)], TN)
        if shard < 128:
            row[:, pl.ds(0, half)] = tile
            tile = row[pl.ds(pl.multiple_of(d * shard - begin, shard), shard), pl.ds(0, half)]
        return tile

    def dw_send_tile(c, j):
        half = chunks[c][3] // 2
        if c > 0:
            s1_copy(c - 1, j).wait_send()
        d = xor(me, 2 * j + 1, z.bits)
        for h in (0, 1):
            send1[j, :, pl.ds(h * half, half)] = tile_of(c, d, h).astype(BF16)
        s1_copy(c, j).start()

    def dw_own_tile(c, j):
        col, width = chunks[c][2:]
        half = width // 2
        d = xor(me, 2 * j, z.bits)
        s1_copy(c, j).wait_recv()
        fetch = pltpu.make_async_copy(land1_o.at[j, :, pl.ds(col, width)], stage1.at[:, pl.ds(0, width)], ld2.at[2])
        fetch.start()
        for h in (0, 1):
            tile = tile_of(c, d, h)
            if h == 0:
                fetch.wait()
            part = part_ref(c, j, col + h * half, half)
            part[...] = (tile + stage1[:, pl.ds(h * half, half)].astype(F32)).astype(BF16)
            for m in kept(z.orders_back[h], 1):
                if m & (1 << z.orders_back[h][1]):
                    @pl.when(2 * j == m)
                    def _():
                        s2_copy(c, h, 1, m, False).start()

    def dw_first():
        def body(i, _):
            dw_send_tile(0, half_n - 1 - i)
            return 0
        lax.fori_loop(0, half_n, body, 0)

    def dw_step(c):
        def body(i, _):
            j = half_n - 1 - i
            if c + 1 < len(chunks):
                dw_send_tile(c + 1, j)
            dw_own_tile(c, j)
            return 0
        lax.fori_loop(0, half_n, body, 0)

    outs = []

    def put(src, dst):
        copy = pltpu.make_async_copy(src, dst, out_sem.at[len(outs)])
        copy.start()
        outs.append(copy)

    def dw_combine(c):
        col, width = chunks[c][2:]
        half = width // 2
        for stage in range(1, z.bits - 1):
            jobs = [(h, m) for h in (0, 1) for m in kept(z.orders_back[h], stage + 1)]
            jobs.sort(key=lambda job: job[1] == 0)

            def fetch(k):
                h, m = jobs[k]
                s2_copy(c, h, stage, m, True).wait_recv()
                source = land2_o.at[slot_of[h][(stage, m)], :, pl.ds(col + h * half, half)]
                copy = pltpu.make_async_copy(source, stage2.at[k % 2, :, pl.ds(0, half)], ld2.at[3 + k % 2])
                copy.start()
                return copy

            ahead = fetch(0)
            for k, (h, m) in enumerate(jobs):
                now = ahead
                if k + 1 < len(jobs):
                    ahead = fetch(k + 1)
                now.wait()
                add_rows(part_ref(c, m >> 1, col + h * half, half), stage2.at[k % 2, :, pl.ds(0, half)], shard)
                if m & (1 << z.orders_back[h][stage + 1]):
                    s2_copy(c, h, stage + 1, m, False).start()
        put(part_ref(c, 0, col, width), own_o.at[:, pl.ds(col, width)])

    def v_copy(m, receive):
        slot = peers.at[flip(me, m)] if receive else peers.at[me]
        return remote(small, slot, vs.at[m], vr.at[m], {"dp": flip(me, m)})

    def t_copy(k, receive):
        to = lax.rem(t + k, nt)
        slot = peers.at[n + (lax.rem(t + nt - k, nt) if receive else t)]
        return remote(tot, slot, ts.at[k], tr.at[k], {"tensor": to})

    def sums_start():
        for m in range(1, n):
            v_copy(m, False).start()

    def sums_over_group():
        for m in range(1, n):
            v_copy(m, True).wait_recv()
        total = small[...]
        for m in range(1, n):
            total = total + peers[flip(me, m)]
        tot[...] = total
        for k in range(1, nt):
            t_copy(k, False).start()
        for m in range(1, n):
            v_copy(m, False).wait_send()

    def sums_over_all():
        for k in range(1, nt):
            t_copy(k, True).wait_recv()
        rest = jnp.zeros(tot.shape, F32)
        for k in range(1, nt):
            rest = rest + peers[n + lax.rem(t + nt - k, nt)]
        at = lax.broadcasted_iota(jnp.int32, tot.shape, 0)
        small[...] = jnp.where(at == 2, small[...], jnp.where(at >= 5, tot[...] + rest, tot[...]))
        for k in range(1, nt):
            t_copy(k, False).wait_send()
        put(small, sums_o)

    def finish_out():
        mine_x = pltpu.make_async_copy(x_hbm, stb, ld2.at[1])
        mine_x.start()
        mine_x.wait()

        def body(i, _):
            at = pl.ds(pl.multiple_of(i * 16, 16), 16)
            own = xs[pl.ds(pl.multiple_of(t * R + i * 16, 16), 16), :].astype(F32)
            total = stb[at, :].astype(F32) + (own + sta[0, at, :].astype(F32) + sta[1, at, :].astype(F32))
            stb[at, :] = (total + small[3:4, :D]).astype(BF16)
            return 0

        lax.fori_loop(0, R // 16, body, 0)
        copy = pltpu.make_async_copy(stb, out_o, ld2.at[1])
        copy.start()
        copy.wait()

    fin_rows = fin.shape[1]

    def finish_grad():
        def out(g):
            return pltpu.make_async_copy(fin.at[g % 2], ig_o.at[pl.ds(g * fin_rows, fin_rows), :], ld2.at[g % 2])

        for g in range(R // fin_rows):
            if g > 1:
                out(g - 2).wait()

            def body(i, _):
                at = pl.ds(pl.multiple_of(g * fin_rows + i * 16, 16), 16)
                rows = pl.ds(pl.multiple_of(t * R + g * fin_rows + i * 16, 16), 16)
                full = stb[at, :].astype(F32)
                centred = full - jnp.mean(full, axis=1, keepdims=True)
                inv_std = lax.rsqrt(jnp.mean(centred * centred, axis=1, keepdims=True) + EPSILON)
                hat = centred * inv_std
                grad = ng[rows, :].astype(F32) + sta[0, at, :].astype(F32) + sta[1, at, :].astype(F32)
                grad = grad * small[2:3, :D]
                middle = jnp.mean(grad, axis=1, keepdims=True)
                along = jnp.mean(grad * hat, axis=1, keepdims=True)
                fin[g % 2, pl.ds(pl.multiple_of(i * 16, 16), 16), :] = cs[rows, :].astype(F32) + inv_std * (grad - middle - hat * along)
                return 0

            lax.fori_loop(0, fin_rows // 16, body, 0)
            out(g).start()
        for g in range(max(0, R // fin_rows - 2), R // fin_rows):
            out(g).wait()

    def w_all_sent():
        for sent in w_sent:
            for copy in sent:
                copy.wait_send()

    def rec_wait():
        for c in range(len(chunks)):
            for h in (0, 1):
                s2_copy(c, h, z.bits - 1, 0, True).wait_recv()

    def all_sent():
        for c in range(len(chunks)):
            for h in (0, 1):
                for stage in range(1, z.bits):
                    for m in kept(z.orders_back[h], stage):
                        if m & (1 << z.orders_back[h][stage]):
                            s2_copy(c, h, stage, m, False).wait_send()
        for j in range(half_n):
            s1_copy(len(chunks) - 1, j).wait_send()
        for m in range(1, n):
            pack_copy(m, False).wait_send()
        z_edges_sent(1)

    per_seq = nt // z.seqs
    mine = t // per_seq
    other = z.seqs - 1 - mine
    pal = t + 1 - 2 * lax.rem(t, 2)
    near = other * per_seq + (per_seq - 1) * (1 - other)
    far = other * per_seq + (per_seq - 1) * other
    vectors()
    layer_norm(t, 0)
    w_step(Q, 0)
    w_start(U, 0)
    x_event(1)
    layer_norm(pal, 1)
    w_step(O, 0)
    w_rest(Q)
    w_ready(Q)
    qkv_tiles(mine)
    w_step(U, 0)
    w_start(Dn, 0)
    attend(mine)
    x_event(2)
    xhat_out(t, 0).wait()
    layer_norm(near, 0)
    w_rest(O)
    w_rest(U)
    x_event(3)
    xhat_out(pal, 1).wait()
    layer_norm(far, 1)
    qkv_tiles(other)
    w_ready(U)
    up_tiles(mine)
    w_step(Dn, 0)
    attend(other)
    c_event(1)
    w_ready(O)
    context_grads(mine * LEN, LEN)
    attend_back(mine)
    up_tiles(other)
    w_rest(Dn)
    line_sent(xs, 0)
    w_ready(Dn)
    branch_tiles(other)
    z_edges(0, range(1, nt - 1))
    c_event(2)
    branch_tiles(mine)
    z_edges(0, [nt - 1])
    hidden_grads(mine * LEN, LEN)
    context_grads(near * R, R)
    hidden_grads(near * R, R)
    cot_sums(mine * LEN, LEN)
    cot_sums(near * R, R)
    xhat_out(near, 0).wait()
    xhat_out(far, 1).wait()
    c_event(3)
    context_grads(far * R, R)
    hidden_grads(far * R, R)
    z_forward(0, 1)
    w_all_sent()
    dw_first()
    dw_step(0)
    dw_step(1)
    dw_step(2)
    z_forward(0, 2)
    dw_combine(0)
    attend_back(other)
    dw_combine(1)
    ng_tiles(other)
    dw_combine(2)
    z_edges(1, range(1, nt - 1))
    ng_tiles(mine)
    z_edges(1, [nt - 1])
    z_last(0)
    finish_out()
    z_edges_sent(0)
    cot_sums(far * R, R)
    dw_step(3)
    sums_start()
    dw_step(4)
    z_forward(1, 1)
    dw_combine(3)
    dw_step(5)
    dw_step(6)
    dw_combine(4)
    sums_over_group()
    z_forward(1, 2)
    dw_combine(5)
    sums_over_all()
    dw_combine(6)
    last_x = pltpu.make_async_copy(x_hbm, stb, ld2.at[1])
    last_x.start()
    last_x.wait()
    line_sent(cs, 1)
    rec_wait()
    z_last(1)
    finish_grad()
    all_sent()
    for copy in outs:
        copy.wait()


def block(z, x, cot, wq, wu, wd, wo, pack):
    shape = lambda s, dt=BF16: jax.ShapeDtypeStruct(s, dt)
    T, W, prows = z.rows, z.n1 + z.n2, pack.shape[0]
    width = max(z.d, z.f)
    half_n = z.n // 2
    nc = len(grad_chunks(z))
    most = max(chunk[3] for chunk in grad_chunks(z))
    n_slots = len(halving_slots(z, 0))
    outs = [shape((z.unit, z.d)), shape((z.unit, z.d), F32), shape((z.shard, W)), shape((z.shard, W)), shape((8, width), F32),
            shape((half_n, z.shard, W)), shape((n_slots, z.shard, W)), shape((2, 2, z.nt - 1, z.unit, z.d)), shape((T, z.d))]
    v = pltpu.VMEM
    sem = pltpu.SemaphoreType.DMA
    scratch = [
        v((z.d, W), BF16), v((T, z.d), BF16), v((T, z.d), BF16), v((T, z.q3), BF16), v((T, z.f), BF16), v((T, z.n1), BF16),
        v((T, z.c), BF16), v((T, z.d), BF16), v((z.n, prows, 128), BF16), v((8, z.d), F32), v((1, z.n1), F32), v((8, width), F32),
        v((half_n, z.shard, most), BF16), v((z.shard, most), BF16), v((2, z.shard, most // 2), BF16), v((2, z.unit, z.d), BF16),
        v((z.unit, z.d), BF16), v((2, 32, z.d), F32), v((8, width), F32), v((z.n + z.nt, 8, width), F32),
        v((128 if z.shard < 128 else 8, most // 2), F32),
        sem((7,)), sem((5,)), sem((nc + 1,)), sem((z.n,)), sem((z.n,)), sem((8 * z.n,)), sem((8 * z.n,)), sem((4 * z.nt,)), sem((4 * z.nt,)),
        sem((nc * half_n,)), sem((nc * half_n,)), sem((nc * 2 * (n_slots + 1),)), sem((nc * 2 * (n_slots + 1),)),
        sem((4 * z.nt,)), sem((4 * z.nt,)), sem((z.n,)), sem((z.n,)), sem((z.nt,)), sem((z.nt,)),
    ]
    return pl.pallas_call(
        functools.partial(block_kernel, z),
        out_shape=outs,
        in_specs=[ANY] * 7 + [VMEM] * 3,
        out_specs=[ANY] * len(outs),
        scratch_shapes=scratch,
        compiler_params=pltpu.CompilerParams(collective_id=0, has_side_effects=True, vmem_limit_bytes=67_043_328),
        name="block_kernel",
    )(x, cot, wq, wu, wd, wo, pack, *(jnp.asarray(p) for p in rotary_rows()))


def packed(z, ln_gain, ln_bias, dense_bias, fc2_bias, fc1_bias, qkv_bias):
    lanes, per, base, frows, qrows = pack_rows(z)
    me = lax.axis_index("dp")
    mine = jnp.arange(z.n)[None, :, None] == me
    def spread(a):
        rows, cols = a.reshape(-1, a.shape[-1]).shape
        return jnp.where(mine, a.reshape(rows, 1, cols), BF16(0)).reshape(-1, 128)
    plain = jnp.concatenate([v.reshape(per, lanes) for v in (ln_gain, ln_bias, dense_bias, fc2_bias)], axis=0)
    if lanes < 128:
        plain = jnp.pad(plain, ((0, 0), (0, 128 - lanes)))
    rows = jnp.concatenate([plain, spread(fc1_bias), spread(qkv_bias)], axis=0)
    return jnp.pad(rows, ((0, -rows.shape[0] % 16), (0, 0)))


def shards(x, ln_gain, ln_bias, qkv_weight, qkv_bias, dense_weight, dense_bias, fc1_weight, fc1_bias, fc2_weight, fc2_bias, cotangent):
    z = Sizes(lax.axis_size("dp"), lax.axis_size("tensor"), x.shape[0], x.shape[1], fc1_weight.shape[1], dense_weight.shape[0])
    pack = packed(z, ln_gain, ln_bias, dense_bias, fc2_bias, fc1_bias, qkv_bias)
    hidden_out, input_grad, own, rec, sums = block(
        z, x, cotangent, qkv_weight.reshape(z.shard, z.q3), fc1_weight, fc2_weight.T, dense_weight.T, pack)[:5]
    dw = own.astype(F32) + rec.astype(F32)
    i, t = lax.axis_index("dp"), lax.axis_index("tensor")
    piece = z.d // (z.n * z.nt)
    cut = lambda r: lax.dynamic_slice(sums, (r, (i * z.nt + t) * piece), (1, piece)).reshape(piece)
    hc = HD // z.n
    fb = lax.dynamic_slice_in_dim(sums[1, :z.f].reshape(-1, HD), i * hc, hc, 1)
    qb = lax.dynamic_slice_in_dim(sums[4, :z.q3].reshape(3, -1, HD), i * hc, hc, 2)
    dbias = cut(0)
    return (hidden_out, input_grad, dw[:, :z.q3].reshape(z.shard, 3, z.c), qb, dw[:, z.n1 + z.f:].T, dbias, dw[:, z.q3:z.n1], fb,
            dw[:, z.n1:z.n1 + z.f].T, dbias, cut(5), cut(6))


def solution(mesh):
    both = ("dp", "tensor")
    placed = (
        P(both, None), P("dp"), P("dp"), P("dp", None, "tensor"), P(None, "tensor", "dp"), P("tensor", "dp"),
        P("dp"), P("dp", "tensor"), P("tensor", "dp"), P("tensor", "dp"), P("dp"), P(both, None),
    )
    given = (
        P(both, None), P(both, None), P("dp", None, "tensor"), P(None, "tensor", "dp"), P("tensor", "dp"), P(both),
        P("dp", "tensor"), P("tensor", "dp"), P("tensor", "dp"), P(both), P(both), P(both),
    )
    return jax.shard_map(shards, mesh=mesh, in_specs=placed, out_specs=given, check_vma=False)
```

```python
import functools
import math

import jax
import jax.numpy as jnp
import numpy as np
from jax import lax
from jax.experimental import pallas as pl
from jax.experimental.pallas import tpu as pltpu
from jax.sharding import PartitionSpec as P

HD = 64
ROT = 32
LEN = 512
EPSILON = 1e-05
GELU_C = math.sqrt(2.0 / math.pi)
F32 = jnp.float32
BF16 = jnp.bfloat16
ANY = pl.BlockSpec(memory_space=pl.ANY)
VMEM = pl.BlockSpec(memory_space=pltpu.VMEM)


def gelu_pair(h):
    square = h * h
    tangent = jnp.tanh(h * (GELU_C + (GELU_C * 0.044715) * square))
    half = 0.5 + 0.5 * tangent
    slope = half + 0.5 * h * (1.0 - tangent * tangent) * (GELU_C + (3.0 * 0.044715 * GELU_C) * square)
    return h * half, slope


def rotary_rows():
    position = np.arange(LEN, dtype=np.float32)
    frequency = (10000.0 ** (-np.arange(0, ROT, 2, dtype=np.float32) / ROT)).astype(np.float32)
    angles = (position[:, None] * frequency[None, :]).astype(np.float32)
    cosine, sine = np.cos(angles).astype(np.float32), np.sin(angles).astype(np.float32)
    return np.tile(np.concatenate([cosine, cosine, sine, sine], axis=1), (1, 2))


def flip(index, mask):
    result, place = index, 1
    while place <= mask:
        if mask & place:
            result = result + (1 - 2 * ((index // place) % 2)) * place
        place *= 2
    return result


def span(bits):
    masks = [0]
    for bit in bits:
        masks = masks + [mask | (1 << bit) for mask in masks]
    return masks


def dot(a, b, dims):
    return lax.dot_general(a, b, (dims, ((), ())), preferred_element_type=F32)


NN, NT, TN = ((1,), (0,)), ((1,), (1,)), ((0,), (0,))


class Sizes:
    def __init__(self, groups, tensor, unit, width, hidden, heads_width):
        self.n, self.nt = groups, tensor
        self.bits = groups.bit_length() - 1
        self.unit, self.d, self.f, self.c = unit, width, hidden, heads_width
        self.rows = unit * tensor
        self.seqs = self.rows // LEN
        self.shard = width // groups
        self.q3 = 3 * heads_width
        self.n1 = self.q3 + hidden
        self.n2 = hidden + heads_width
        self.orders = (
            list(range(1, self.bits)) + [0],
            list(range(self.bits - 1, 0, -1)) + [0],
        )
        self.orders_back = tuple(list(reversed(order)) for order in self.orders)


def pack_rows(z):
    lanes = min(128, z.shard)
    per = z.shard // lanes
    return lanes, per, 4 * per, z.f // 128, z.q3 // 128


def rotated(tile, table, sign, turn=True):
    lane = lax.broadcasted_iota(jnp.int32, table.shape, 1) % HD
    sine = pltpu.roll(table, 128 - ROT, axis=1) * sign
    here = jnp.where((lane < ROT) & turn, table, 1.0)
    above = jnp.where((lane < ROT // 2) & turn, -sine, 0.0)
    below = jnp.where((lane >= ROT // 2) & (lane < ROT) & turn, sine, 0.0)
    width = tile.shape[1]
    up = pltpu.roll(tile, width - ROT // 2, axis=1)
    down = pltpu.roll(tile, ROT // 2, axis=1)
    wide = lambda a: jnp.tile(a, (1, width // 128))
    return tile * wide(here) + up * wide(above) + down * wide(below)


def xor(a, b, bits):
    result = 0
    for j in range(bits):
        result = result + (((a // (1 << j)) + (b // (1 << j))) % 2) * (1 << j)
    return result


def kept(order, stage):
    free = [b for b in order[stage:]]
    return sorted(span(free))


def halving_slots(z, h):
    slots = {}
    for stage in range(1, z.bits - 1):
        for m in kept(z.orders_back[h], stage + 1):
            slots[(stage, m)] = len(slots)
    return slots


def grad_chunks(z):
    def cut(kind, at, col, width):
        pieces, start = [], 0
        while start < width:
            size = min(1024, width - start)
            pieces.append((kind, at + start, col + start, size))
            start += size
        return pieces
    return cut("act", 0, z.n1, z.f) + cut("ctx", 0, z.n1 + z.f, z.c) + cut("left", z.q3, z.q3, z.f) + cut("left", 0, 0, z.q3)


def block_kernel(z, *refs):
    (x_hbm, c_hbm, wq_hbm, wu_hbm, wd_hbm, wo_hbm, pack_hbm, table,
     out_o, ig_o, own_q, own_u, own_d, own_p, rec_q, rec_u, rec_d, rec_p, sums_o, land1_o, land2_o, landz_o, xhat_o,
     w, xs, cs, qkv, act, left, ctx, nm, slots, vec, bias, small, send1, stage1, stage2, sta, stb, fin, factor, tot, peers, row,
     loc, ld2, out_sem, pk_send, pk_recv, w_send, w_recv, z_send, z_recv, s1s, s1r, s2s, s2r, zs, zr, vs, vr, ts, tr) = refs
    ng = act
    n, nt, R, D, T = z.n, z.nt, z.unit, z.d, z.rows
    half_n, shard, last = n // 2, z.shard, z.bits - 1
    me, t = lax.axis_index("dp"), lax.axis_index("tensor")
    chunks = grad_chunks(z)

    def remote(src, dst, send, recv, where):
        return pltpu.make_async_remote_copy(
            src_ref=src, dst_ref=dst, send_sem=send, recv_sem=recv, device_id=where, device_id_type=pl.DeviceIdType.MESH
        )

    def rows_of(u):
        return pl.ds(pl.multiple_of(u * R, R), R)

    def seq_rows(seq):
        return pl.ds(pl.multiple_of(seq * LEN, LEN), LEN)

    barrier = pltpu.get_barrier_semaphore()
    for m in range(1, n):
        pl.semaphore_signal(barrier, inc=1, device_id={"dp": flip(me, m)}, device_id_type=pl.DeviceIdType.MESH)
    for step in range(1, nt):
        pl.semaphore_signal(barrier, inc=1, device_id={"tensor": lax.rem(t + step, nt)}, device_id_type=pl.DeviceIdType.MESH)

    wchunks = [(wq_hbm, 0, z.q3), (wo_hbm, z.n1 + z.f, z.c), (wu_hbm, z.q3, z.f), (wd_hbm, z.n1, z.f)]
    Q, O, U, Dn = range(4)

    def slot_ref(d, col, width):
        return w.at[pl.ds(pl.multiple_of(d * shard, shard), shard), pl.ds(col, width)]

    own_copies = [
        pltpu.make_async_copy(x_hbm, xs.at[rows_of(t), :], loc.at[0]),
        pltpu.make_async_copy(c_hbm, cs.at[rows_of(t), :], loc.at[1]),
        pltpu.make_async_copy(pack_hbm, slots.at[me], loc.at[2]),
    ] + [pltpu.make_async_copy(src, slot_ref(me, col, width), loc.at[3 + c]) for c, (src, col, width) in enumerate(wchunks)]
    for copy in own_copies:
        copy.start()
    pl.semaphore_wait(barrier, n - 1 + nt - 1)

    def w_copy(c, h, bit, m, receive):
        src_hbm, col, width = wchunks[c]
        half = width // 2
        col = col + h * half
        d = flip(me, m | (1 << bit)) if receive else flip(me, m)
        dst = slot_ref(d, col, half)
        src = src_hbm.at[:, pl.ds(h * half, half)] if m == 0 and not receive else dst
        s = (c * 2 + h) * n + (m | (1 << bit))
        return remote(src, dst, w_send.at[s], w_recv.at[s], {"dp": flip(me, 1 << bit)})

    w_sent = [[] for _ in wchunks]

    def w_start(c, stage):
        for h in (0, 1):
            order = z.orders[h]
            sends = [(order[stage], m) for m in span(order[:stage])] if stage < last else []
            fresh = [0] if stage == 0 else [m for m in span(order[:stage]) if m & (1 << order[stage - 1])]
            for bit, m in sends + [(0, m) for m in fresh]:
                copy = w_copy(c, h, bit, m, False)
                copy.start()
                w_sent[c].append(copy)

    def w_step(c, stage):
        for h in (0, 1):
            for m in span(z.orders[h][:stage]):
                w_copy(c, h, z.orders[h][stage], m, True).wait_recv()
        w_start(c, stage + 1)

    def w_rest(c):
        for stage in range(1, last):
            w_step(c, stage)

    def w_ready(c):
        for h in (0, 1):
            for m in span(z.orders[h][:last]):
                w_copy(c, h, 0, m, True).wait_recv()

    def pack_copy(m, receive):
        slot = slots.at[flip(me, m)] if receive else slots.at[me]
        return remote(pack_hbm, slot, pk_send.at[m], pk_recv.at[m], {"dp": flip(me, m)})

    def line(buf, which, j, up, receive):
        src = (t - (j - 1)) if up else (t + (j - 1))
        got = (t - j) if up else (t + j)
        ref = buf.at[rows_of(got if receive else src), :]
        s = (which * 2 + (0 if up else 1)) * nt + j
        from_ref = (x_hbm if which == 0 else c_hbm) if j == 1 and not receive else ref
        return remote(from_ref, ref, z_send.at[s], z_recv.at[s], {"tensor": (t + 1) if up else (t - 1)})

    def sends(j, up):
        return ((t < nt - 1) & (t >= j - 1)) if up else ((t > 0) & (t <= nt - j))

    def gets(j, up):
        return (t >= j) if up else (t <= nt - 1 - j)

    def line_send(buf, which, j, up, extra=None):
        cond = sends(j, up) if extra is None else sends(j, up) & extra

        @pl.when(cond)
        def _():
            line(buf, which, j, up, False).start()

    def line_recv(buf, which, j, up):
        @pl.when(gets(j, up))
        def _():
            line(buf, which, j, up, True).wait_recv()

    def line_sent(buf, which):
        for j in range(1, nt):
            for up in (True, False):
                @pl.when(sends(j, up))
                def _():
                    line(buf, which, j, up, False).wait_send()

    def cot_starts(j):
        line_send(cs, 1, 1, True, t == j)
        line_send(cs, 1, 1, False, t == nt - 1 - j)

    def x_event(j):
        for up in (True, False):
            line_recv(xs, 0, j, up)
        if j < nt - 1:
            for up in (True, False):
                line_send(xs, 0, j + 1, up)
        cot_starts(j)

    def c_event(j):
        for up in (True, False):
            line_recv(cs, 1, j, up)
        if j < nt - 1:
            for up in (True, False):
                line_send(cs, 1, j + 1, up)

    for m in range(1, n):
        pack_copy(m, False).start()
    for up in (True, False):
        line_send(xs, 0, 1, up)
    w_start(Q, 0)
    w_start(O, 0)
    cot_starts(0)
    for m in range(1, n):
        pack_copy(m, True).wait_recv()
    for copy in own_copies:
        copy.wait()

    lanes, per, base, frows, qrows = pack_rows(z)

    def vectors():
        small[...] = jnp.zeros_like(small)
        for v in range(4):
            for d in range(n):
                for r in range(per):
                    at = d * shard + r * lanes
                    vec[pl.ds(v, 1), pl.ds(at, lanes)] = slots[d, pl.ds(v * per + r, 1), :lanes].astype(F32)
        total = jnp.zeros((frows + qrows, 128), F32)
        for d in range(n):
            total = total + slots[d, pl.ds(base, frows + qrows), :].astype(F32)
        for r in range(qrows):
            bias[:, pl.ds(r * 128, 128)] = total[frows + r:frows + r + 1, :]
        for r in range(frows):
            bias[:, pl.ds(z.q3 + r * 128, 128)] = total[r:r + 1, :]
        small[2:3, :D] = vec[0:1, :]
        small[3:4, :D] = vec[2:3, :] + vec[3:4, :]

    def xhat_out(u, slot):
        return pltpu.make_async_copy(sta.at[slot], xhat_o.at[rows_of(u), :], ld2.at[slot])

    def layer_norm(u, slot):
        block = 16

        def body(i, _):
            at = pl.ds(pl.multiple_of(i * block, block), block)
            rows = pl.ds(pl.multiple_of(u * R + i * block, block), block)
            full = xs[rows, :].astype(F32)
            centred = full - jnp.mean(full, axis=1, keepdims=True)
            inv_std = lax.rsqrt(jnp.mean(centred * centred, axis=1, keepdims=True) + EPSILON)
            hat = centred * inv_std
            sta[slot, at, :] = hat.astype(BF16)
            nm[rows, :] = (hat * vec[0:1, :] + vec[1:2, :]).astype(BF16)
            return 0

        lax.fori_loop(0, R // block, body, 0)
        xhat_out(u, slot).start()

    def qkv_tiles(seq):
        rows = seq_rows(seq)

        def body(part, _):
            cols = pl.ds(pl.multiple_of(part * z.c, z.c), z.c)
            tile = dot(nm[rows, :], w[:, cols], NN) + bias[:, cols]
            qkv[rows, cols] = rotated(tile, table[...], 1.0, part < 2).astype(BF16)
            return 0

        lax.fori_loop(0, 3, body, 0)

    def up_tiles(seq):
        rows = seq_rows(seq)

        def body(j, _):
            cols = pl.ds(pl.multiple_of(j * 512, 512), 512)
            wcols = pl.ds(pl.multiple_of(z.q3 + j * 512, 512), 512)
            value, slope = gelu_pair(dot(nm[rows, :], w[:, wcols], NN) + bias[:, wcols])
            act[rows, cols] = value.astype(BF16)
            left[rows, wcols] = slope.astype(BF16)
            return 0

        lax.fori_loop(0, z.f // 512, body, 0)

    half_rows = LEN // 2

    def head_pair(seq, p):
        def block(part, start, count):
            cols = pl.ds(pl.multiple_of(part * z.c + p * 128, 128), 128)
            return qkv[pl.ds(pl.multiple_of(seq * LEN + start, half_rows), count), cols]
        return block

    def softmax(q2, k2, keep, start):
        keys = k2.shape[0]
        row_at = lax.broadcasted_iota(jnp.int32, (half_rows, keys), 0) + start
        seen = lax.broadcasted_iota(jnp.int32, (half_rows, keys), 1) <= row_at
        scores = jnp.where(seen, dot(jnp.where(keep, q2 * BF16(0.125), BF16(0)), k2, NT), -1e30)
        e = jnp.exp(scores - jnp.max(scores, axis=1, keepdims=True))
        return e * (1.0 / jnp.sum(e, axis=1, keepdims=True))

    def attend(seq):
        low = lax.broadcasted_iota(jnp.int32, (half_rows, 128), 1) < HD

        def pair(p, _):
            block = head_pair(seq, p)
            for qb in range(2):
                start, keys = qb * half_rows, half_rows * (qb + 1)
                q2, k2, v2 = block(0, start, half_rows), block(1, 0, keys), block(2, 0, keys)
                parts = [dot(softmax(q2, k2, keep, start).astype(BF16), v2, NN) for keep in (low, ~low)]
                ctx[pl.ds(pl.multiple_of(seq * LEN + start, half_rows), half_rows),
                    pl.ds(pl.multiple_of(p * 128, 128), 128)] = jnp.where(low, parts[0], parts[1]).astype(BF16)
            return 0

        lax.fori_loop(0, z.c // 128, pair, 0)

    def branch_tiles(seq):
        rows = seq_rows(seq)

        def body(j, _):
            wrows = pl.ds(pl.multiple_of(j * 512, 512), 512)
            tile = dot(act[rows, :], w[wrows, pl.ds(z.n1, z.f)], NT)
            tile = tile + dot(ctx[rows, :], w[wrows, pl.ds(z.n1 + z.f, z.c)], NT)
            xs[rows, wrows] = tile.astype(BF16)
            return 0

        lax.fori_loop(0, D // 512, body, 0)

    def context_grads(begin, count):
        rows = pl.ds(pl.multiple_of(begin, count), count)
        left[rows, pl.ds(2 * z.c, z.c)] = dot(cs[rows, :], w[:, pl.ds(z.n1 + z.f, z.c)], NN).astype(BF16)

    def hidden_grads(begin, count):
        rows = pl.ds(pl.multiple_of(begin, count), count)

        def body(j, _):
            cols = pl.ds(pl.multiple_of(j * 512, 512), 512)
            gcols = pl.ds(pl.multiple_of(z.q3 + j * 512, 512), 512)
            wcols = pl.ds(pl.multiple_of(z.n1 + j * 512, 512), 512)
            grad = dot(cs[rows, :], w[:, wcols], NN) * left[rows, gcols].astype(F32)
            small[1:2, cols] += jnp.sum(grad, axis=0, keepdims=True)
            left[rows, gcols] = grad.astype(BF16)
            return 0

        lax.fori_loop(0, z.f // 512, body, 0)

    def cot_sums(begin, count):
        def sums(i, _):
            part = cs[pl.ds(pl.multiple_of(begin + i * 64, 64), 64), :].astype(F32)
            small[0:1, :D] += jnp.sum(part, axis=0, keepdims=True)
            return 0

        lax.fori_loop(0, count // 64, sums, 0)

    def unit_grads(u):
        hidden_grads(u * R, R)
        cot_sums(u * R, R)
        return 0

    def attend_back(seq):
        low = lax.broadcasted_iota(jnp.int32, (half_rows, 128), 1) < HD
        low_all = lax.broadcasted_iota(jnp.int32, (LEN, 128), 1) < HD

        def pair(p, _):
            block = head_pair(seq, p)
            gcols = pl.ds(pl.multiple_of(2 * z.c + p * 128, 128), 128)
            dqs, dks, dvs = [], [None, None], [None, None]
            for qb in range(2):
                start, keys = qb * half_rows, half_rows * (qb + 1)
                q2, k2, v2 = block(0, start, half_rows), block(1, 0, keys), block(2, 0, keys)
                g2 = left[pl.ds(pl.multiple_of(seq * LEN + start, half_rows), half_rows), gcols]
                dq = []
                for side, keep in enumerate((low, ~low)):
                    prob = softmax(q2, k2, keep, start)
                    grad = dot(jnp.where(keep, g2, BF16(0)), v2, NT)
                    delta = jnp.sum(prob * grad, axis=1, keepdims=True)
                    ds = (prob * (grad - delta) * 0.125).astype(BF16)
                    dq.append(dot(ds, k2, NN))
                    dk = dot(ds, q2, TN)
                    dv = dot(prob.astype(BF16), g2, TN)
                    if qb:
                        zero = jnp.zeros((half_rows, 128), F32)
                        dk = dk + jnp.concatenate([dks[side], zero], axis=0)
                        dv = dv + jnp.concatenate([dvs[side], zero], axis=0)
                    dks[side], dvs[side] = dk, dv
                dqs.append(jnp.where(low, dq[0], dq[1]))
            grads = (jnp.concatenate(dqs, axis=0), jnp.where(low_all, dks[0], dks[1]), jnp.where(low_all, dvs[0], dvs[1]))
            for which, value in enumerate(grads):
                if which < 2:
                    value = rotated(value, table[...], -1.0)
                cols = pl.ds(pl.multiple_of(which * z.c + p * 128, 128), 128)
                small[4:5, cols] += jnp.sum(value, axis=0, keepdims=True)
                left[seq_rows(seq), cols] = value.astype(BF16)
            return 0

        lax.fori_loop(0, z.c // 128, pair, 0)

    def ng_tiles(seq):
        rows = seq_rows(seq)

        def hat(j):
            slot = lax.rem(j, 2) if not isinstance(j, int) else j % 2
            cols = pl.ds(pl.multiple_of(j * 512, 512), 512)
            place = ctx.at[pl.ds(pl.multiple_of(slot * LEN, LEN), LEN), :]
            return place, pltpu.make_async_copy(xhat_o.at[rows, cols], place, ld2.at[slot])

        hat(0)[1].start()

        def body(j, _):
            cols = pl.ds(pl.multiple_of(j * 512, 512), 512)

            @pl.when(j + 1 < D // 512)
            def _():
                hat(j + 1)[1].start()
            tile = dot(left[rows, :], w[cols, pl.ds(0, z.n1)], NT)
            place, copy = hat(j)
            copy.wait()
            small[5:6, cols] += jnp.sum(tile * place[...].astype(F32), axis=0, keepdims=True)
            small[6:7, cols] += jnp.sum(tile, axis=0, keepdims=True)
            ng[rows, cols] = tile.astype(BF16)
            return 0

        lax.fori_loop(0, D // 512, body, 0)

    def place_of(up):
        return t if up else nt - 1 - t

    def real_unit(u, up):
        return u if up else nt - 1 - u

    def z_copy(phase, up, k, src):
        i = (phase * 2 + (0 if up else 1)) * nt + k
        slot = landz_o.at[phase, 0 if up else 1, k - 1]
        return remote(slot if src is None else src, slot, zs.at[i], zr.at[i], {"tensor": (t + 1) if up else (t - 1)})

    def z_own(phase, u):
        return (xs if phase == 0 else ng).at[rows_of(u), :]

    def z_edges(phase, which):
        for k in which:
            for up in (True, False):
                @pl.when(place_of(up) == 0)
                def _():
                    z_copy(phase, up, k, z_own(phase, real_unit(nt - k, up))).start()

    def add_rows(dst, src, rows, block=32):
        def body(i, _):
            at = pl.ds(pl.multiple_of(i * block, block), block)
            dst[at, :] = (dst[at, :].astype(F32) + src[at, :].astype(F32)).astype(BF16)
            return 0
        lax.fori_loop(0, rows // block, body, 0)

    def z_take(phase, k, up, a):
        e = place_of(up)
        if k > 1:
            @pl.when(e <= k - 1)
            def _():
                z_copy(phase, up, k, a).wait_send()
        z_copy(phase, up, k, None).wait_recv()
        got = pltpu.make_async_copy(landz_o.at[phase, 0 if up else 1, k - 1], a, ld2.at[0])
        got.start()
        got.wait()

    def z_forward(phase, k):
        for up in (True, False):
            e = place_of(up)
            a = sta.at[0 if up else 1]

            @pl.when((e >= 1) & (e <= k))
            def _():
                z_take(phase, k, up, a)
                add_rows(a, z_own(phase, real_unit(nt - 1 + e - k, up)), R)
                z_copy(phase, up, k + 1, a).start()

    def z_last(phase):
        for up in (True, False):
            a = sta.at[0 if up else 1]

            @pl.when(place_of(up) >= 1)
            def _():
                z_take(phase, nt - 1, up, a)

            @pl.when(place_of(up) < 1)
            def _():
                a[...] = jnp.zeros_like(a)

    def z_edges_sent(phase):
        for up in (True, False):
            for k in range(1, nt):
                @pl.when(place_of(up) == 0)
                def _():
                    z_copy(phase, up, k, z_own(phase, real_unit(nt - k, up))).wait_send()

    slot_of = [halving_slots(z, h) for h in (0, 1)]
    n_slots = len(slot_of[0])

    def part_ref(c, j, cols, width):
        kind, at = chunks[c][:2]
        if kind != "left":
            buf, first, shift = w, 0, 0
        elif at >= z.q3:
            buf, first, shift = w, D // 2, z.n1 - z.q3
        else:
            buf, first, shift = xs, 0, 0
        begin = first + j * shard
        if not isinstance(j, int):
            begin = pl.multiple_of(begin, shard)
        return buf.at[pl.ds(begin, shard), pl.ds(cols + shift, width)]

    def home(c, refs):
        kind, at = chunks[c][:2]
        which = {"act": 2, "ctx": 3}[kind] if kind != "left" else (1 if at >= z.q3 else 0)
        return refs[which], (0, z.q3, z.n1, z.n1 + z.f)[which]

    owns, recs = (own_q, own_u, own_d, own_p), (rec_q, rec_u, rec_d, rec_p)

    def s1_copy(c, j):
        col, width = chunks[c][2:]
        i = c * half_n + j
        return remote(send1.at[j, :, pl.ds(0, width)], land1_o.at[j, :, pl.ds(col, width)], s1s.at[i], s1r.at[i], {"dp": flip(me, 1)})

    def s2_copy(c, h, stage, m, receive):
        col, width = chunks[c][2:]
        half = width // 2
        at = col + h * half
        bit = z.orders_back[h][stage]
        kept_m = m if receive else m & ~(1 << bit)
        final = stage == z.bits - 1
        slot = n_slots if final else slot_of[h][(stage, kept_m)]
        if final:
            ref, begin = home(c, recs)
            dst = ref.at[:, pl.ds(at - begin, half)]
        else:
            dst = land2_o.at[slot, :, pl.ds(at, half)]
        src = dst if receive else part_ref(c, m >> 1, at, half)
        i = (c * 2 + h) * (n_slots + 1) + slot
        return remote(src, dst, s2s.at[i], s2r.at[i], {"dp": flip(me, 1 << bit)})

    block = max(shard, 128)

    def tile_of(c, d, h):
        kind, at, col, width = chunks[c]
        half = width // 2
        begin = d * shard
        if shard < 128:
            begin = (begin // 128) * 128
        cols = pl.ds(pl.multiple_of(begin, 128), block)
        buf = {"act": act, "ctx": ctx, "left": left}[kind]
        tile = dot((nm if kind == "left" else cs)[:, cols], buf[:, pl.ds(at + h * half, half)], TN)
        if shard < 128:
            row[:, pl.ds(0, half)] = tile
            tile = row[pl.ds(pl.multiple_of(d * shard - begin, shard), shard), pl.ds(0, half)]
        return tile

    def dw_send_tile(c, j):
        half = chunks[c][3] // 2
        if c > 0:
            s1_copy(c - 1, j).wait_send()
        d = xor(me, 2 * j + 1, z.bits)
        for h in (0, 1):
            send1[j, :, pl.ds(h * half, half)] = tile_of(c, d, h).astype(BF16)
        s1_copy(c, j).start()

    def dw_fetch(c, j):
        col, width = chunks[c][2:]
        s1_copy(c, j).wait_recv()
        fetch = pltpu.make_async_copy(land1_o.at[j, :, pl.ds(col, width)], stage1.at[:, pl.ds(0, width)], ld2.at[2])
        fetch.start()
        return fetch

    def dw_own_tile(c, j, fetch):
        col, width = chunks[c][2:]
        half = width // 2
        d = xor(me, 2 * j, z.bits)
        for h in (0, 1):
            tile = tile_of(c, d, h)
            if h == 0:
                fetch.wait()
            part = part_ref(c, j, col + h * half, half)
            part[...] = (tile + stage1[:, pl.ds(h * half, half)].astype(F32)).astype(BF16)
            for m in kept(z.orders_back[h], 1):
                if m & (1 << z.orders_back[h][1]):
                    @pl.when(2 * j == m)
                    def _():
                        s2_copy(c, h, 1, m, False).start()

    def dw_first():
        def body(i, _):
            dw_send_tile(0, half_n - 1 - i)
            return 0
        lax.fori_loop(0, half_n, body, 0)

    def dw_step(c):
        def body(i, _):
            j = half_n - 1 - i
            fetch = dw_fetch(c, j)
            if c + 1 < len(chunks):
                dw_send_tile(c + 1, j)
            dw_own_tile(c, j, fetch)
            return 0
        lax.fori_loop(0, half_n, body, 0)

    outs = []

    def put(src, dst):
        copy = pltpu.make_async_copy(src, dst, out_sem.at[len(outs)])
        copy.start()
        outs.append(copy)

    def dw_combine(c):
        col, width = chunks[c][2:]
        half = width // 2
        for stage in range(1, z.bits - 1):
            jobs = [(h, m) for h in (0, 1) for m in kept(z.orders_back[h], stage + 1)]
            jobs.sort(key=lambda job: job[1] == 0)

            def fetch(k):
                h, m = jobs[k]
                s2_copy(c, h, stage, m, True).wait_recv()
                source = land2_o.at[slot_of[h][(stage, m)], :, pl.ds(col + h * half, half)]
                copy = pltpu.make_async_copy(source, stage2.at[k % 2, :, pl.ds(0, half)], ld2.at[3 + k % 2])
                copy.start()
                return copy

            ahead = fetch(0)
            for k, (h, m) in enumerate(jobs):
                now = ahead
                if k + 1 < len(jobs):
                    ahead = fetch(k + 1)
                now.wait()
                add_rows(part_ref(c, m >> 1, col + h * half, half), stage2.at[k % 2, :, pl.ds(0, half)], shard)
                if m & (1 << z.orders_back[h][stage + 1]):
                    s2_copy(c, h, stage + 1, m, False).start()
        ref, begin = home(c, owns)
        put(part_ref(c, 0, col, width), ref.at[:, pl.ds(col - begin, width)])

    def v_copy(m, receive):
        slot = peers.at[flip(me, m)] if receive else peers.at[me]
        return remote(small, slot, vs.at[m], vr.at[m], {"dp": flip(me, m)})

    def t_copy(k, receive):
        to = lax.rem(t + k, nt)
        slot = peers.at[n + (lax.rem(t + nt - k, nt) if receive else t)]
        return remote(tot, slot, ts.at[k], tr.at[k], {"tensor": to})

    def sums_start():
        for m in range(1, n):
            v_copy(m, False).start()

    def sums_over_group():
        for m in range(1, n):
            v_copy(m, True).wait_recv()
        total = small[...]
        for m in range(1, n):
            total = total + peers[flip(me, m)]
        tot[...] = total
        for k in range(1, nt):
            t_copy(k, False).start()
        for m in range(1, n):
            v_copy(m, False).wait_send()

    def sums_over_all():
        for k in range(1, nt):
            t_copy(k, True).wait_recv()
        rest = jnp.zeros(tot.shape, F32)
        for k in range(1, nt):
            rest = rest + peers[n + lax.rem(t + nt - k, nt)]
        at = lax.broadcasted_iota(jnp.int32, tot.shape, 0)
        small[...] = jnp.where(at == 2, small[...], jnp.where(at >= 5, tot[...] + rest, tot[...]))
        for k in range(1, nt):
            t_copy(k, False).wait_send()
        put(small, sums_o)

    def finish_out():
        mine_x = pltpu.make_async_copy(x_hbm, stb, ld2.at[1])
        mine_x.start()
        mine_x.wait()

        def body(i, _):
            at = pl.ds(pl.multiple_of(i * 16, 16), 16)
            own = xs[pl.ds(pl.multiple_of(t * R + i * 16, 16), 16), :].astype(F32)
            total = stb[at, :].astype(F32) + (own + sta[0, at, :].astype(F32) + sta[1, at, :].astype(F32))
            stb[at, :] = (total + small[3:4, :D]).astype(BF16)
            return 0

        lax.fori_loop(0, R // 16, body, 0)
        copy = pltpu.make_async_copy(stb, out_o, ld2.at[1])
        copy.start()
        copy.wait()

    def prepare_grad():
        copy = pltpu.make_async_copy(x_hbm, stb, ld2.at[1])
        copy.start()
        copy.wait()

        def body(i, _):
            at = pl.ds(pl.multiple_of(i * 16, 16), 16)
            full = stb[at, :].astype(F32)
            centred = full - jnp.mean(full, axis=1, keepdims=True)
            inv_std = lax.rsqrt(jnp.mean(centred * centred, axis=1, keepdims=True) + EPSILON)
            stb[at, :] = (centred * inv_std).astype(BF16)
            factor[at, :] = jnp.broadcast_to(inv_std, (16, 128))
            return 0

        lax.fori_loop(0, R // 16, body, 0)

    fin_rows = fin.shape[1]

    def finish_grad():
        def out(g):
            return pltpu.make_async_copy(fin.at[g % 2], ig_o.at[pl.ds(g * fin_rows, fin_rows), :], ld2.at[g % 2])

        for g in range(R // fin_rows):
            if g > 1:
                out(g - 2).wait()

            def body(i, _):
                at = pl.ds(pl.multiple_of(g * fin_rows + i * 16, 16), 16)
                rows = pl.ds(pl.multiple_of(t * R + g * fin_rows + i * 16, 16), 16)
                hat = stb[at, :].astype(F32)
                inv_std = factor[at, 0:1]
                grad = ng[rows, :].astype(F32) + sta[0, at, :].astype(F32) + sta[1, at, :].astype(F32)
                grad = grad * small[2:3, :D]
                middle = jnp.mean(grad, axis=1, keepdims=True)
                along = jnp.mean(grad * hat, axis=1, keepdims=True)
                fin[g % 2, pl.ds(pl.multiple_of(i * 16, 16), 16), :] = cs[rows, :].astype(F32) + inv_std * (grad - middle - hat * along)
                return 0

            lax.fori_loop(0, fin_rows // 16, body, 0)
            out(g).start()
        for g in range(max(0, R // fin_rows - 2), R // fin_rows):
            out(g).wait()

    def w_all_sent():
        for sent in w_sent:
            for copy in sent:
                copy.wait_send()

    def rec_wait():
        for c in range(len(chunks)):
            for h in (0, 1):
                s2_copy(c, h, z.bits - 1, 0, True).wait_recv()

    def all_sent():
        for c in range(len(chunks)):
            for h in (0, 1):
                for stage in range(1, z.bits):
                    for m in kept(z.orders_back[h], stage):
                        if m & (1 << z.orders_back[h][stage]):
                            s2_copy(c, h, stage, m, False).wait_send()
        for j in range(half_n):
            s1_copy(len(chunks) - 1, j).wait_send()
        for m in range(1, n):
            pack_copy(m, False).wait_send()
        z_edges_sent(1)

    per_seq = nt // z.seqs
    mine = t // per_seq
    other = z.seqs - 1 - mine
    pal = t + 1 - 2 * lax.rem(t, 2)
    near = other * per_seq + (per_seq - 1) * (1 - other)
    far = other * per_seq + (per_seq - 1) * other
    def both(first, second, work, between):
        def body(i, _):
            work(jnp.where(i == 0, first, second))
            for k in (0, 1):
                pl.when(i == k)(between[k])
            return 0

        lax.fori_loop(0, 2, body, 0)

    def after_branch():
        z_edges(0, range(1, nt - 1))
        c_event(2)

    def after_ng():
        z_edges(1, range(1, nt - 1))

    vectors()
    layer_norm(t, 0)
    w_step(Q, 0)
    w_start(U, 0)
    x_event(1)
    layer_norm(pal, 1)
    w_step(O, 0)
    w_rest(Q)
    w_ready(Q)
    qkv_tiles(mine)
    w_step(U, 0)
    w_start(Dn, 0)
    attend(mine)
    x_event(2)
    xhat_out(t, 0).wait()
    layer_norm(near, 0)
    w_rest(O)
    w_rest(U)
    x_event(3)
    xhat_out(pal, 1).wait()
    layer_norm(far, 1)
    qkv_tiles(other)
    w_ready(U)
    up_tiles(mine)
    w_step(Dn, 0)
    attend(other)
    c_event(1)
    w_ready(O)
    context_grads(mine * LEN, LEN)
    attend_back(mine)
    up_tiles(other)
    w_rest(Dn)
    line_sent(xs, 0)
    w_ready(Dn)
    both(other, mine, branch_tiles, (after_branch, lambda: z_edges(0, [nt - 1])))
    context_grads(near * R, R)
    lax.fori_loop(0, per_seq + 1, lambda i, _: unit_grads(jnp.where(i < per_seq, mine * per_seq + i, near)), 0)
    xhat_out(near, 0).wait()
    xhat_out(far, 1).wait()
    c_event(3)
    context_grads(far * R, R)
    unit_grads(far)
    w_all_sent()
    dw_first()
    z_forward(0, 1)
    dw_step(0)
    dw_step(1)
    dw_step(2)
    z_forward(0, 2)
    dw_combine(0)
    attend_back(other)
    dw_combine(1)
    both(other, mine, ng_tiles, (after_ng, lambda: z_edges(1, [nt - 1])))
    dw_combine(2)
    z_last(0)
    finish_out()
    z_edges_sent(0)
    sums_start()
    dw_step(3)
    z_forward(1, 1)
    dw_step(4)
    dw_combine(3)
    dw_step(5)
    dw_step(6)
    sums_over_group()
    dw_combine(4)
    z_forward(1, 2)
    dw_combine(5)
    dw_combine(6)
    prepare_grad()
    line_sent(cs, 1)
    sums_over_all()
    rec_wait()
    z_last(1)
    finish_grad()
    all_sent()
    for copy in outs:
        copy.wait()


def block(z, x, cot, wq, wu, wd, wo, pack):
    shape = lambda s, dt=BF16: jax.ShapeDtypeStruct(s, dt)
    T, W, prows = z.rows, z.n1 + z.n2, pack.shape[0]
    width = max(z.d, z.f)
    half_n = z.n // 2
    nc = len(grad_chunks(z))
    most = max(chunk[3] for chunk in grad_chunks(z))
    n_slots = len(halving_slots(z, 0))
    outs = [shape((z.unit, z.d)), shape((z.unit, z.d), F32)] + [shape((z.shard, k)) for k in (z.q3, z.f, z.f, z.c)] * 2 + [shape((8, width), F32),
            shape((half_n, z.shard, W)), shape((n_slots, z.shard, W)), shape((2, 2, z.nt - 1, z.unit, z.d)), shape((T, z.d))]
    v = pltpu.VMEM
    sem = pltpu.SemaphoreType.DMA
    scratch = [
        v((z.d, W), BF16), v((T, z.d), BF16), v((T, z.d), BF16), v((T, z.q3), BF16), v((T, z.f), BF16), v((T, z.n1), BF16),
        v((T, z.c), BF16), v((T, z.d), BF16), v((z.n, prows, 128), BF16), v((8, z.d), F32), v((1, z.n1), F32), v((8, width), F32),
        v((half_n, z.shard, most), BF16), v((z.shard, most), BF16), v((2, z.shard, most // 2), BF16), v((2, z.unit, z.d), BF16),
        v((z.unit, z.d), BF16), v((2, 32, z.d), F32), v((z.unit, 128), F32), v((8, width), F32), v((z.n + z.nt, 8, width), F32),
        v((128 if z.shard < 128 else 8, most // 2), F32),
        sem((7,)), sem((5,)), sem((nc + 1,)), sem((z.n,)), sem((z.n,)), sem((8 * z.n,)), sem((8 * z.n,)), sem((4 * z.nt,)), sem((4 * z.nt,)),
        sem((nc * half_n,)), sem((nc * half_n,)), sem((nc * 2 * (n_slots + 1),)), sem((nc * 2 * (n_slots + 1),)),
        sem((4 * z.nt,)), sem((4 * z.nt,)), sem((z.n,)), sem((z.n,)), sem((z.nt,)), sem((z.nt,)),
    ]
    return pl.pallas_call(
        functools.partial(block_kernel, z),
        out_shape=outs,
        in_specs=[ANY] * 7 + [VMEM],
        out_specs=[ANY] * len(outs),
        scratch_shapes=scratch,
        compiler_params=pltpu.CompilerParams(collective_id=0, has_side_effects=True, vmem_limit_bytes=67_043_328),
        name="block_kernel",
    )(x, cot, wq, wu, wd, wo, pack, jnp.asarray(rotary_rows()))


def packed(z, ln_gain, ln_bias, dense_bias, fc2_bias, fc1_bias, qkv_bias):
    lanes, per, base, frows, qrows = pack_rows(z)
    me = lax.axis_index("dp")
    mine = jnp.arange(z.n)[None, :, None] == me
    def spread(a):
        rows, cols = a.reshape(-1, a.shape[-1]).shape
        return jnp.where(mine, a.reshape(rows, 1, cols), BF16(0)).reshape(-1, 128)
    plain = jnp.concatenate([v.reshape(per, lanes) for v in (ln_gain, ln_bias, dense_bias, fc2_bias)], axis=0)
    if lanes < 128:
        plain = jnp.pad(plain, ((0, 0), (0, 128 - lanes)))
    rows = jnp.concatenate([plain, spread(fc1_bias), spread(qkv_bias)], axis=0)
    return jnp.pad(rows, ((0, -rows.shape[0] % 16), (0, 0)))


def shards(x, ln_gain, ln_bias, qkv_weight, qkv_bias, dense_weight, dense_bias, fc1_weight, fc1_bias, fc2_weight, fc2_bias, cotangent):
    z = Sizes(lax.axis_size("dp"), lax.axis_size("tensor"), x.shape[0], x.shape[1], fc1_weight.shape[1], dense_weight.shape[0])
    pack = packed(z, ln_gain, ln_bias, dense_bias, fc2_bias, fc1_bias, qkv_bias)
    hidden_out, input_grad, oq, ou, od, op, rq, ru, rd, rp, sums = block(
        z, x, cotangent, qkv_weight.reshape(z.shard, z.q3), fc1_weight, fc2_weight.T, dense_weight.T, pack)[:11]
    add = lambda a, b: a.astype(F32) + b.astype(F32)
    i, t = lax.axis_index("dp"), lax.axis_index("tensor")
    piece = z.d // (z.n * z.nt)
    cut = lambda r: lax.dynamic_slice(sums, (r, (i * z.nt + t) * piece), (1, piece)).reshape(piece)
    hc = HD // z.n
    fb = lax.dynamic_slice_in_dim(sums[1, :z.f].reshape(-1, HD), i * hc, hc, 1)
    qb = lax.dynamic_slice_in_dim(sums[4, :z.q3].reshape(3, -1, HD), i * hc, hc, 2)
    dbias = cut(0)
    return (hidden_out, input_grad, add(oq, rq).reshape(z.shard, 3, z.c), qb, add(op, rp).T, dbias, add(ou, ru), fb,
            add(od, rd).T, dbias, cut(5), cut(6))


def solution(mesh):
    both = ("dp", "tensor")
    placed = (
        P(both, None), P("dp"), P("dp"), P("dp", None, "tensor"), P(None, "tensor", "dp"), P("tensor", "dp"),
        P("dp"), P("dp", "tensor"), P("tensor", "dp"), P("tensor", "dp"), P("dp"), P(both, None),
    )
    given = (
        P(both, None), P(both, None), P("dp", None, "tensor"), P(None, "tensor", "dp"), P("tensor", "dp"), P(both),
        P("dp", "tensor"), P("tensor", "dp"), P("tensor", "dp"), P(both), P(both), P(both),
    )
    return jax.shard_map(shards, mesh=mesh, in_specs=placed, out_specs=given, check_vma=False)
```
